32 devices in a mesh: dp: 2 (over x), expert: 16 (over z, y, core).
Axes of the slice: x: 2, y: 2, z: 4, core: 2. Of those that a mesh axis runs over, the one named last changes fastest.
Arguments:
- tokens: bfloat16 [4096, 2048], P(('dp', 'expert')), may hold values from -160 to 160
- router_weight: bfloat16 [2048, 16], replicated, may hold values from -0.25 to 0.25
- route_ids: int32 [4096, 2], P(('dp', 'expert')), may hold values from 0 to 15, as said below
- gate_weight: bfloat16 [16, 768, 2048], P('expert', 'dp'), may hold values from -0.125 to 0.125
- up_weight: bfloat16 [16, 768, 2048], P('expert', 'dp'), may hold values from -0.125 to 0.125
- down_weight: bfloat16 [16, 768, 2048], P('expert', 'dp'), may hold values from -0.21875 to 0.21875
Outputs:
- mixture: bfloat16 [4096, 2048], P(('dp', 'expert'))
- z_loss: float32 [], replicated
The draws below stay inside these ranges and needn't reach their ends.
Inputs may be any that keep to these rules, and one draw needn't show every extreme that they name: `route_ids`: each row names 2 different experts; among the rows of one device no expert is named more than 20 times, and one expert is named exactly 20 times by the rows of every device.
All inputs are finite; a program needn't handle non-finite values.
Results may differ from the reference program's by a relative error of at most 0.0057.
Values may be sent and summed in bfloat16 or wider, within the bound.
A program may use at most 64 MiB of HBM per device.

```python
import math
import jax
import jax.numpy as jnp
from jax import lax

D = 2048
FF = 768
EXP_DEV = 1
TOPK = 2
TOK_DEV = 128
EXPERTS = 16
CAP = 20
TOKENS = 4096


def router_table(key):
    base_key = jax.random.fold_in(key, 7)
    bound_value = math.sqrt(3.0 / D)
    values = jax.random.uniform(base_key, (D, EXPERTS), jnp.float32, -bound_value, bound_value)
    return values.astype(jnp.bfloat16).astype(jnp.float32)


def expert_order(subkey):
    return jax.random.permutation(subkey, EXPERTS)


def token_order(subkey):
    return jax.random.permutation(subkey, TOK_DEV)


def route_table(key):
    blocks = TOKENS // TOK_DEV
    slots_dev = TOK_DEV * TOPK
    base_count = slots_dev // EXPERTS
    spare = CAP - base_count
    half_count = EXPERTS // 2
    key_pairs, key_moves, key_order, key_rows = jax.random.split(jax.random.fold_in(key, 3), 4)
    pairing = jax.random.permutation(key_pairs, EXPERTS)
    moves = jax.random.randint(key_moves, (blocks, half_count), 0, spare + 1)
    moves = moves.at[:, 0].set(spare)
    paired = jnp.stack([base_count + moves, base_count - moves], axis=2).reshape(blocks, EXPERTS)
    counts = jnp.zeros((blocks, EXPERTS), jnp.int32).at[:, pairing].set(paired.astype(jnp.int32))
    orders = jax.vmap(expert_order)(jax.random.split(key_order, blocks))
    ordered_counts = jnp.take_along_axis(counts, orders, axis=1)
    bounds = jnp.cumsum(ordered_counts, axis=1)
    slot_pos = jnp.arange(slots_dev, dtype=jnp.int32)
    run_index = jnp.sum((bounds[:, None, :] <= slot_pos[None, :, None]).astype(jnp.int32), axis=2)
    expert_at = jnp.take_along_axis(orders, run_index, axis=1)
    route_grid = expert_at.reshape(blocks, TOPK, TOK_DEV).transpose(0, 2, 1)
    shuffles = jax.vmap(token_order)(jax.random.split(key_rows, blocks))
    route_grid = jnp.take_along_axis(route_grid, shuffles[:, :, None], axis=1)
    return route_grid.reshape(TOKENS, TOPK).astype(jnp.int32)


def close_gaps(values, router, routes, target_key):
    logits = jnp.dot(values, router, precision=lax.Precision.HIGHEST)
    expert_ids = jnp.arange(EXPERTS, dtype=jnp.int32)[None, :]
    first_hot = (routes[:, 0:1] == expert_ids).astype(jnp.float32)
    second_hot = (routes[:, 1:2] == expert_ids).astype(jnp.float32)
    diff_hot = first_hot - second_hot
    current_gap = jnp.sum(logits * diff_hot, axis=1)
    gram = jnp.dot(router.T, router, precision=lax.Precision.HIGHEST)
    diff_norm = jnp.sum(jnp.dot(diff_hot, gram, precision=lax.Precision.HIGHEST) * diff_hot, axis=1)
    target_gap = jax.random.uniform(target_key, (TOKENS,), jnp.float32, -2.5, 2.5)
    coefficient = (target_gap - current_gap) / diff_norm
    shift_rows = jnp.dot(coefficient[:, None] * diff_hot, router.T, precision=lax.Precision.HIGHEST)
    return values + shift_rows


def draw_router_weight(key, part):
    return router_table(key).astype(jnp.bfloat16)


def draw_route_ids(key, part):
    return route_table(key)


def draw_tokens(key, part):
    blocks = TOKENS // TOK_DEV
    groups = EXPERTS // EXP_DEV
    lanes = blocks // groups
    device = jnp.arange(TOKENS) // TOK_DEV
    along = (device % groups).astype(jnp.float32) / max(groups - 1, 1)
    across = (device // groups).astype(jnp.float32) / max(lanes - 1, 1)
    ramp_scale = (0.5 + 2.3 * along) * (1.0 + across)
    key_noise, key_scale = jax.random.split(jax.random.fold_in(key, 5), 2)
    key_target = jax.random.fold_in(key, 11)
    router = router_table(key)
    routes = route_table(key)
    spread = jnp.exp(jax.random.uniform(key_scale, (TOKENS,), jnp.float32, math.log(0.6), math.log(1.6)))
    noise_part = jax.random.normal(key_noise, (TOKENS, D), jnp.float32)
    values = noise_part * (ramp_scale * spread)[:, None]
    values = close_gaps(values, router, routes, key_target)
    return jnp.clip(values, -160.0, 160.0).astype(jnp.bfloat16)


def block_scale(key, shape, shards, smallest, top_value):
    loudness = 1.0
    for axis_at, shards_of in shards:
        heights = jax.random.uniform(jax.random.fold_in(jax.random.fold_in(key, 6), axis_at), (shards_of,), jnp.float32, smallest / len(shards), top_value / len(shards))
        loudness = loudness * jnp.repeat(jnp.exp(heights), shape[axis_at] // shards_of).reshape((-1,) + (1,) * (len(shape) - 1 - axis_at))
    return loudness


def scatter_about(stream_key, dims, scale, reach, cuts=(), kind=jnp.bfloat16):
    entries = jax.random.normal(stream_key, dims, jnp.float32) * scale
    if len(cuts) > 0:
        entries = block_scale(stream_key, dims, cuts, -0.22, 0.18) * entries
    return jnp.clip(entries, min=-reach, max=reach).astype(kind)


def setup_inputs(seed: int = 0) -> dict:
    keys = jax.random.split(jax.random.key(seed), 7)
    tokens = draw_tokens(jax.random.fold_in(keys[6], 71), 0)
    router_weight = draw_router_weight(jax.random.fold_in(keys[6], 71), 0)
    route_ids = draw_route_ids(jax.random.fold_in(keys[6], 71), 0)
    gate_weight = scatter_about(keys[3], (EXPERTS, FF, D), D ** -0.5, 0.125, ((0, 16), (1, 2)))
    up_weight = scatter_about(keys[4], (EXPERTS, FF, D), D ** -0.5, 0.125, ((0, 16), (1, 2)))
    down_weight = scatter_about(keys[5], (EXPERTS, FF, D), FF ** -0.5, 0.21875, ((0, 16), (1, 2)))
    return {"tokens": tokens, "router_weight": router_weight, "route_ids": route_ids, "gate_weight": gate_weight, "up_weight": up_weight, "down_weight": down_weight}


def block_tables(ids_block, weights_block):
    flat_ids = ids_block.reshape(-1)
    onehot = (flat_ids[:, None] == jnp.arange(EXPERTS, dtype=jnp.int32)[None, :]).astype(jnp.int32)
    before = jnp.cumsum(onehot, axis=0) - onehot
    position = jnp.sum(before * onehot, axis=1)
    slots = flat_ids * CAP + position
    slot_match = slots[None, :] == jnp.arange(EXPERTS * CAP, dtype=jnp.int32)[:, None]
    token_of = jnp.arange(TOK_DEV * TOPK, dtype=jnp.int32) // TOPK
    source_row = jnp.sum(jnp.where(slot_match, token_of[None, :], 0), axis=1).astype(jnp.int32)
    filled = jnp.any(slot_match, axis=1)
    flat_weights = weights_block.reshape(-1)
    slot_weight = jnp.sum(jnp.where(slot_match, flat_weights[None, :], jnp.zeros((), flat_weights.dtype)), axis=1)
    return source_row, filled, slot_weight


def tables_of(block_pair):
    return block_tables(block_pair[0], block_pair[1])


def reference(tokens, router_weight, route_ids, gate_weight, up_weight, down_weight):
    logits = jnp.dot(tokens, router_weight, preferred_element_type=jnp.float32)
    log_total = jax.nn.logsumexp(logits, axis=1)
    z_loss = jnp.mean(log_total * log_total)
    chosen = jnp.take_along_axis(logits, route_ids, axis=1)
    route_weight = jax.nn.softmax(chosen, axis=1)
    blocks = TOKENS // TOK_DEV
    source_row, filled, slot_weight = lax.map(tables_of, (route_ids.reshape(blocks, TOK_DEV, TOPK), route_weight.reshape(blocks, TOK_DEV, TOPK)))
    offsets = (jnp.arange(blocks, dtype=jnp.int32) * TOK_DEV)[:, None]
    global_row = (source_row + offsets).astype(jnp.int32)

    def by_expert(table):
        return table.reshape(blocks, EXPERTS, CAP).transpose(1, 0, 2).reshape(EXPERTS, blocks * CAP)

    def expert_step(accumulated, inputs):
        gate_one, up_one, down_one, rows_one, filled_one, weight_one = inputs
        expert_rows = jnp.where(filled_one[:, None], tokens[rows_one], jnp.zeros((), tokens.dtype))
        rows_wide = expert_rows.astype(jnp.float32)
        gate_val = jnp.dot(rows_wide, gate_one.astype(jnp.float32).T, preferred_element_type=jnp.float32)
        up_val = jnp.dot(rows_wide, up_one.astype(jnp.float32).T, preferred_element_type=jnp.float32)
        hidden = (jax.nn.silu(gate_val) * up_val).astype(jnp.bfloat16)
        expert_out = jnp.dot(hidden.astype(jnp.float32), down_one.astype(jnp.float32), preferred_element_type=jnp.float32).astype(jnp.bfloat16)
        accumulated = accumulated.at[rows_one].add(weight_one[:, None] * expert_out.astype(jnp.float32))
        return accumulated, None

    initial = jnp.zeros((TOKENS, D), jnp.float32)
    accumulated, unused = lax.scan(expert_step, initial, (gate_weight, up_weight, down_weight, by_expert(global_row), by_expert(filled), by_expert(slot_weight)))
    return accumulated.astype(jnp.bfloat16), z_loss
```

```python
import functools

import jax
import jax.numpy as jnp
from jax import lax
from jax.experimental import pallas as pl
from jax.experimental.pallas import tpu as pltpu
from jax.sharding import PartitionSpec as P

MESH = pl.DeviceIdType.MESH
F32 = jnp.float32
BF16 = jnp.bfloat16
TILE = 16
NO = None
PLAN = (
    ("send", 0), ("send", 2), ("send", 1), ("send", 3),
    ("load", 0), ("got", 0), ("own", 0),
    ("got", (1, 2), 0), ("got", (1, 2), 1), ("route", 0), ("got", (1, 2), 2), ("got", (1, 2), 3),
    ("own", (1, 2)), ("peer", 0),
    ("got", (2, 1), 0), ("got", (2, 1), 1), ("got", (2, 1), 2), ("got", (2, 1), 3),
    ("own", (2, 1)), ("weigh", 0), ("peer", (1, 2)), ("part", (NO, 2)),
    ("got", (3, NO), 0), ("got", (3, NO), 1), ("got", (3, NO), 2), ("got", (3, NO), 3),
    ("peer", (2, 1)), ("part", (2, NO)),
    ("got", (NO, 3), 0), ("got", (NO, 3), 1), ("end", (NO, 2)), ("got", (NO, 3), 2), ("got", (NO, 3), 3),
    ("part", (NO, 1)), ("own", 3), ("peer", 3), ("part", 3), ("part", (1, NO)), ("part", 0),
    ("end", (2, NO)), ("end", (3, 1)), ("loss", 0), ("done", (2,)), ("end", (1, 3)), ("end", 0),
    ("drain", 0), ("done", (1, 3)), ("done", (0,)),
)
PLAN_ONE = tuple(
    (op, (0,) if op == "done" else 0)
    for op in ("send", "load", "got", "route", "weigh", "own", "peer", "part", "end", "loss", "drain", "done")
)


def dot(a, b, dims=((1,), (0,))):
    return lax.dot_general(a, b, (dims, ((), ())), preferred_element_type=F32)


def iota(shape, axis):
    return lax.broadcasted_iota(jnp.int32, shape, axis)


def kernel(
    n, dpn, cap, groups,
    tok_ref, router_ref, ids_ref, gate_hbm, up_hbm, down_hbm,
    mix_ref, z_ref,
    snd, rx, px, fin, ret, own, gate_ref, up_ref, down_ref, zsnd, zrx, zmid, zdp,
    d_send, d_recv, f_send, f_recv, p_send, p_recv, r_send, r_recv,
    z_send, z_recv, y_send, y_recv, w_sem,
    hi_ref, lo_ref, w_ref, acc_ref,
):
    rows, width = tok_ref.shape
    topk = ids_ref.shape[0]
    size = n // groups
    mains = cap // TILE
    rest = cap - mains * TILE
    slot = 1
    while slot < rest:
        slot *= 2
    cuts = TILE // slot
    part = width // cuts
    base = mains * width
    me = lax.axis_index("expert")
    dp = lax.axis_index("dp")
    zone = me // size
    lane = me % size

    plan = PLAN if groups == 4 else PLAN_ONE
    inner = ((zone + 1) // 2) % 2 if groups == 4 else 0
    first_send = [step[1] for step in plan if step[0] == "send"][0]
    tail = [step[1] for step in plan if step[0] == "done"]

    def home(k):
        return isinstance(k, int) and k == 0

    def zone_of(k):
        if groups == 4:
            return ((zone // 2 + k // 2) % 2) * 2 + (zone % 2 + k % 2) % 2
        return (zone + k) % groups

    def peer_of(j):
        return (dp + j) % dpn

    loads = [
        pltpu.make_async_copy(src.at[0], dst, w_sem.at[i])
        for i, (src, dst) in enumerate(
            ((gate_hbm, gate_ref), (up_hbm, up_ref), (down_hbm, down_ref))
        )
    ]
    for load in loads:
        load.start()

    barrier = pltpu.get_barrier_semaphore()

    def greet(j, c):
        pl.semaphore_signal(
            barrier, inc=1, device_id={"expert": (me + j) % n}, device_id_type=MESH
        )
        return c

    lax.fori_loop(1, n, greet, 0)
    for j in range(1, dpn):
        pl.semaphore_signal(
            barrier, inc=1, device_id={"dp": peer_of(j)}, device_id_type=MESH
        )

    with jax.named_scope("begin"):
        pass
    hot_t = [(ids_ref[k : k + 1, :] == iota((n, rows), 0)) for k in range(topk)]
    all_t = sum(h.astype(F32) for h in hot_t).astype(BF16)
    upper = (iota((rows, rows), 0) < iota((rows, rows), 1)).astype(F32).astype(BF16)
    before_t = dot(all_t, upper)
    pos_t = [
        jnp.sum(jnp.where(h, before_t, 0.0), axis=0, keepdims=True).astype(jnp.int32)
        for h in hot_t
    ]

    def targets(ids, pos):
        out = []
        for m in range(mains):
            inside = (pos >= m * TILE) & (pos < (m + 1) * TILE)
            out.append(jnp.where(inside, ids * TILE + pos - m * TILE, -1))
        for c in range(cuts if rest else 0):
            inside = pos >= mains * TILE
            out.append(jnp.where(inside, ids * TILE + c * slot + pos - mains * TILE, -1))
        return out

    goal_t = [targets(ids_ref[k : k + 1, :], pos_t[k]) for k in range(topk)]
    row_at = iota((size * TILE, rows), 0)

    def dispatch(to, at):
        return pltpu.make_async_remote_copy(
            src_ref=snd.at[to], dst_ref=rx.at[dp, at],
            send_sem=d_send.at[to], recv_sem=d_recv.at[at],
            device_id={"expert": to}, device_id_type=MESH,
        )

    def forward(j, at, whose):
        return pltpu.make_async_remote_copy(
            src_ref=rx.at[dp, at], dst_ref=rx.at[whose, at],
            send_sem=f_send.at[peer_of(j), at], recv_sem=f_recv.at[whose, at],
            device_id={"dp": peer_of(j)}, device_id_type=MESH,
        )

    def send_group(k):
        first = zone_of(k) * size
        mine = pl.ds(first, size)

        def pick(i):
            at = row_at + first * TILE
            hit = at == goal_t[0][i]
            for c in range(1, topk):
                hit = hit | (at == goal_t[c][i])
            return hit.astype(F32).astype(BF16)

        for m in range(mains):
            snd[mine, :, m * width : (m + 1) * width] = (
                dot(pick(m), tok_ref[...]).astype(BF16).reshape(size, TILE, width)
            )
        if rest:
            extra = sum(
                dot(pick(mains + c), tok_ref[:, c * part : (c + 1) * part])
                for c in range(cuts)
            )
            snd[mine, :, base:] = extra.astype(BF16).reshape(size, TILE, part)
        if k == first_send:
            pl.semaphore_wait(barrier, n - 1 + dpn - 1)

        def one(j, c):
            to = first + (lane + j) % size
            dispatch(to, me).start()
            return c

        lax.fori_loop(1 if home(k) else 0, size, one, 0)
        if k == 0:
            rx[dp, me] = snd[me]
            for q in range(1, dpn):
                forward(q, me, dp).start()

    count = size * TILE
    at_row, at_col = iota((count, count), 0), iota((count, count), 1)
    per_cut = size * slot
    want = ((at_row % per_cut) // slot) * TILE + (at_row // per_cut) * slot + at_row % slot
    order = (at_col == want).astype(F32).astype(BF16)

    def natural(block):
        pieces = [
            block[:, :, m * width : (m + 1) * width].reshape(count, width)
            for m in range(mains)
        ]
        if rest:
            sorted_rows = dot(order, block[:, :, base:].reshape(count, part)).astype(BF16)
            pieces.append(
                jnp.concatenate(
                    [sorted_rows[c * per_cut : (c + 1) * per_cut] for c in range(cuts)],
                    axis=1,
                )
            )
        return pieces

    def blocks_of(rows_out, store):
        for m in range(mains):
            store(
                m * width, width,
                rows_out[m * count : (m + 1) * count].reshape(size, TILE, width),
            )
        if rest:
            tail = rows_out[mains * count :]
            stacked = jnp.concatenate(
                [tail[:, c * part : (c + 1) * part] for c in range(cuts)], axis=0
            )
            mixed = dot(order, stacked, ((0,), (0,))).astype(BF16)
            store(base, part, mixed.reshape(size, TILE, part))

    def expert(block):
        x = jnp.concatenate(natural(block), axis=0)
        gate = dot(x, gate_ref[...], ((1,), (1,)))
        up = dot(x, up_ref[...], ((1,), (1,)))
        hidden = (gate / (1.0 + jnp.exp(-gate)) * up).astype(BF16)
        return dot(hidden, down_ref[...])

    def partial_copy(j, t, whose):
        first = zone_of(t) * size
        return pltpu.make_async_remote_copy(
            src_ref=rx.at[peer_of(j), pl.ds(first, size)],
            dst_ref=px.at[whose, pl.ds(first, size)],
            send_sem=p_send.at[peer_of(j), t], recv_sem=p_recv.at[whose, t],
            device_id={"dp": peer_of(j)}, device_id_type=MESH,
        )

    def give_back(to, at):
        return pltpu.make_async_remote_copy(
            src_ref=fin.at[to], dst_ref=ret.at[at],
            send_sem=r_send.at[to], recv_sem=r_recv.at[at],
            device_id={"expert": to}, device_id_type=MESH,
        )

    def loss_copy(to, at):
        return pltpu.make_async_remote_copy(
            src_ref=zsnd, dst_ref=zrx.at[at],
            send_sem=z_send.at[to], recv_sem=z_recv.at[at],
            device_id={"expert": to}, device_id_type=MESH,
        )

    def loss_dp(j, whose):
        return pltpu.make_async_remote_copy(
            src_ref=zmid, dst_ref=zdp.at[whose],
            send_sem=y_send.at[peer_of(j)], recv_sem=y_recv.at[whose],
            device_id={"dp": peer_of(j)}, device_id_type=MESH,
        )

    def route():
        logits = dot(tok_ref[...], router_ref[...], ((1,), (1,)))
        top = jnp.max(logits, axis=1, keepdims=True)
        log_total = top + jnp.log(jnp.sum(jnp.exp(logits - top), axis=1, keepdims=True))
        local = jnp.sum(log_total * log_total, axis=0, keepdims=True)
        zsnd[...] = jnp.broadcast_to(local, zsnd.shape)
        zrx[me] = jnp.broadcast_to(local, zsnd.shape)

        def send_loss(j, c):
            loss_copy((me + j) % n, me).start()
            return c

        lax.fori_loop(1, n, send_loss, 0)

        same = (iota((n, n), 0) == iota((n, n), 1)).astype(F32).astype(BF16)
        hot = [dot(h.astype(F32).astype(BF16), same, ((0,), (0,))) > 0.5 for h in hot_t]
        ids = [
            jnp.sum(jnp.where(h, iota((rows, n), 1), 0), axis=1, keepdims=True) for h in hot
        ]
        chosen = [jnp.sum(jnp.where(h, logits, 0.0), axis=1, keepdims=True) for h in hot]
        high = functools.reduce(jnp.maximum, chosen)
        exps = [jnp.exp(c - high) for c in chosen]
        share = [e / sum(exps) for e in exps]
        all_hot = sum(h.astype(F32) for h in hot).astype(BF16)
        lower = (iota((rows, rows), 1) < iota((rows, rows), 0)).astype(F32).astype(BF16)
        before = dot(lower, all_hot)
        pos = [
            jnp.sum(jnp.where(h, before, 0.0), axis=1, keepdims=True).astype(jnp.int32)
            for h in hot
        ]
        goal = [targets(ids[k], pos[k]) for k in range(topk)]

        col_at = iota((rows, n * TILE), 1)
        for i in range(mains + (cuts if rest else 0)):
            w = sum(jnp.where(col_at == goal[k][i], share[k], 0.0) for k in range(topk))
            hi = w.astype(BF16)
            hi_ref[i] = hi
            lo_ref[i] = (w - hi.astype(F32)).astype(BF16)

    def arrive(k, part=None):
        first = zone_of(k) * size

        def one(j, c):
            at = first + (lane + size - j) % size
            dispatch(at, at).wait_recv()
            for q in range(1, dpn):
                forward(q, at, dp).start()
            return c

        if part is None:
            lax.fori_loop(1 if home(k) else 0, size, one, 0)
        else:
            quarter = size // 4
            lax.fori_loop(part * quarter, (part + 1) * quarter, one, 0)

    def own_part(k):
        own[k] = expert(rx[dp, pl.ds(zone_of(k) * size, size)])

    def peer_part(k):
        first = zone_of(k) * size

        def one(q, c):
            whose = peer_of(q)

            def landed(j, c2):
                forward(q, first + (lane + j) % size, whose).wait_recv()
                return c2

            lax.fori_loop(0, size, landed, 0)
            out = expert(rx[whose, pl.ds(first, size)]).astype(BF16)

            def store(start, wide, value):
                rx[whose, pl.ds(first, size), :, start : start + wide] = value

            blocks_of(out, store)
            return c

        lax.fori_loop(1, dpn, one, 0)

    def send_part(k):
        for q in range(1, dpn):
            partial_copy(q, k, dp).start()

    def finish(k):
        first = zone_of(k) * size
        total = own[k]
        for q in range(1, dpn):
            partial_copy(q, k, peer_of(q)).wait_recv()
            block = px[peer_of(q), pl.ds(first, size)]
            total = total + jnp.concatenate(natural(block), axis=0).astype(F32)

        def store(start, wide, value):
            fin[pl.ds(first, size), :, start : start + wide] = value

        blocks_of(total.astype(BF16), store)

        def back(j, c):
            give_back(first + (lane + j) % size, me).start()
            return c

        lax.fori_loop(1 if home(k) else 0, size, back, 0)
        if home(k):
            ret[me] = fin[me]

    def cut(i, k):
        start = zone_of(k) * size * TILE
        sub = (iota((n * TILE, size * TILE), 0) == iota((n * TILE, size * TILE), 1) + start)
        sub = sub.astype(F32).astype(BF16)
        hi = dot(hi_ref[i], sub).astype(BF16)
        lo = dot(lo_ref[i], sub).astype(BF16)
        return jnp.concatenate([hi, lo], axis=1)

    def weigh(k):
        for i in range(mains + (cuts if rest else 0)):
            for k in range(groups):
                w_ref[i, k] = cut(i, k)

    def take(ks):
        for k in ks:
            first = zone_of(k) * size

            def one(j, c, first=first):
                at = first + (lane + size - j) % size
                give_back(at, at).wait_recv()
                return c

            lax.fori_loop(1 if home(k) else 0, size, one, 0)

        def twice(x):
            return jnp.concatenate([x, x], axis=0)

        for c in range(cuts):
            cols = slice(c * part, (c + 1) * part)
            acc = 0.0 if ks == tail[0] else acc_ref[:, cols]
            for k in ks:
                mine = pl.ds(zone_of(k) * size, size)
                for m in range(mains):
                    seen = ret[mine, :, m * width + c * part : m * width + (c + 1) * part]
                    acc = acc + dot(w_ref[m, k], twice(seen.reshape(count, part)))
                if rest:
                    seen = ret[mine, :, base:].reshape(count, part)
                    acc = acc + dot(w_ref[mains + c, k], twice(seen))
            if ks == tail[-1]:
                mix_ref[:, cols] = acc.astype(BF16)
            else:
                acc_ref[:, cols] = acc

    def loads_in(k):
        for load in loads:
            load.wait()

    def gather_loss():
        def loss_in(j, c):
            at = (me + j) % n
            loss_copy(at, at).wait_recv()
            return c

        lax.fori_loop(1, n, loss_in, 0)
        mid = zrx[0]
        for i in range(1, n):
            mid = mid + zrx[i]
        zmid[...] = mid
        zdp[dp] = mid

        for q in range(1, dpn):
            loss_dp(q, dp).start()

    def drain(k):
        def sent(j, c):
            to = (me + j) % n
            dispatch(to, me).wait_send()
            loss_copy(to, me).wait_send()
            return c

        lax.fori_loop(1, n, sent, 0)
        for q in range(1, dpn):
            loss_dp(q, dp).wait_send()

            def forwarded(at, c, q=q):
                forward(q, at, dp).wait_send()
                return c

            lax.fori_loop(0, n, forwarded, 0)

            def parted(t, c, q=q):
                partial_copy(q, t, dp).wait_send()
                return c

            lax.fori_loop(0, groups, parted, 0)
        loss = zdp[dp]
        for q in range(1, dpn):
            loss_dp(q, peer_of(q)).wait_recv()
            loss = loss + zdp[peer_of(q)]
        z_ref[...] = loss[0:1, 0:1] / F32(rows * n * dpn)

    steps = {
        "send": send_group, "got": arrive, "own": own_part, "peer": peer_part,
        "part": send_part, "end": finish, "done": take, "load": loads_in,
        "route": lambda k: route(), "loss": lambda k: gather_loss(), "weigh": weigh, "drain": drain,
    }
    for op, at, *more in plan:
        with jax.named_scope(f"{op}_{at}_{more}"):
            if op == "done" or not isinstance(at, tuple):
                steps[op](at, *more)
            elif None in at:
                chosen = at[0] if at[1] is None else at[1]
                pl.when(inner == at.index(chosen))(functools.partial(steps[op], chosen, *more))
            else:
                steps[op](at[0] + inner * (at[1] - at[0]), *more)

    def returned(j, c):
        give_back((me + j) % n, me).wait_send()
        return c

    with jax.named_scope("finalwait"):
        lax.fori_loop(1, n, returned, 0)


def on_device(n, dpn, tokens, router_weight, route_ids, gate_weight, up_weight, down_weight):
    rows, width = tokens.shape
    topk = route_ids.shape[1]
    experts = router_weight.shape[1]
    assert experts == n and gate_weight.shape[0] == 1
    cap = 5 * rows * topk // (4 * experts)
    groups = 4 if n % 4 == 0 else 1
    mains, rest = cap // TILE, cap % TILE
    slot = 1
    while slot < rest:
        slot *= 2
    block = mains * width + (width * slot // TILE if rest else 0)
    size = n // groups
    in_rows = size * TILE * mains + (size * slot if rest else 0)
    hidden = gate_weight.shape[1]
    vmem = pl.BlockSpec(memory_space=pltpu.VMEM)
    hbm = pl.BlockSpec(memory_space=pl.ANY)
    dma = pltpu.SemaphoreType.DMA
    mixture, loss = pl.pallas_call(
        functools.partial(kernel, n, dpn, cap, groups),
        out_shape=(
            pltpu.VMEM((rows, width), BF16),
            jax.ShapeDtypeStruct((1, 1), F32),
        ),
        in_specs=[vmem, vmem, vmem, hbm, hbm, hbm],
        out_specs=(vmem, vmem),
        scratch_shapes=[
            pltpu.VMEM((n, TILE, block), BF16),
            pltpu.VMEM((dpn, n, TILE, block), BF16),
            pltpu.VMEM((dpn, n, TILE, block), BF16),
            pltpu.VMEM((n, TILE, block), BF16),
            pltpu.VMEM((n, TILE, block), BF16),
            pltpu.VMEM((groups, in_rows, width), F32),
            pltpu.VMEM((hidden, width), BF16),
            pltpu.VMEM((hidden, width), BF16),
            pltpu.VMEM((hidden, width), BF16),
            pltpu.VMEM((8, 128), F32),
            pltpu.VMEM((n, 8, 128), F32),
            pltpu.VMEM((8, 128), F32),
            pltpu.VMEM((dpn, 8, 128), F32),
            dma((n,)), dma((n,)), dma((dpn, n)), dma((dpn, n)),
            dma((dpn, groups)), dma((dpn, groups)), dma((n,)), dma((n,)),
            dma((n,)), dma((n,)), dma((dpn,)), dma((dpn,)), dma((3,)),
            pltpu.VMEM((mains + (TILE // slot if rest else 0), rows, n * TILE), BF16),
            pltpu.VMEM((mains + (TILE // slot if rest else 0), rows, n * TILE), BF16),
            pltpu.VMEM((mains + (TILE // slot if rest else 0), groups, rows, 2 * size * TILE), BF16),
            pltpu.VMEM((rows, width), F32),
        ],
        compiler_params=pltpu.CompilerParams(
            collective_id=0, has_side_effects=True, vmem_limit_bytes=60 * 1024 * 1024
        ),
    )(tokens, router_weight.T, route_ids.T, gate_weight, up_weight, down_weight)
    return mixture, loss[0, 0]


def solution(mesh):
    in_specs = (
        P(("dp", "expert"), None),
        P(),
        P(("dp", "expert"), None),
        P("expert", "dp", None),
        P("expert", "dp", None),
        P("expert", "dp", None),
    )
    out_specs = (P(("dp", "expert"), None), P())
    return jax.shard_map(
        functools.partial(on_device, mesh.shape["expert"], mesh.shape["dp"]),
        mesh=mesh, in_specs=in_specs, out_specs=out_specs, check_vma=False,
    )
```

```python
import functools

import jax
import jax.numpy as jnp
from jax import lax
from jax.experimental import pallas as pl
from jax.experimental.pallas import tpu as pltpu
from jax.sharding import PartitionSpec as P

MESH = pl.DeviceIdType.MESH
F32 = jnp.float32
BF16 = jnp.bfloat16
TILE = 16
NO = None
PLAN = (
    ("send", (2, 1), True), ("send", 0), ("send", (1, 2)), ("send", 3),
    ("load", 0), ("got", 0), ("own", 0),
    ("got", (1, 2), 0), ("got", (1, 2), 1), ("route", 0), ("got", (1, 2), 2), ("got", (1, 2), 3),
    ("own", (1, 2)), ("peer", 0),
    ("got", (2, 1), 0), ("got", (2, 1), 1),
    ("weigh", 0), ("peer", (1, 2)), ("part", (NO, 2)),
    ("got", (2, NO), 2), ("got", (2, NO), 3), ("own", (2, NO)),
    ("got", 3, 0), ("got", 3, 1), ("got", 3, 2), ("got", 3, 3),
    ("peer", (2, NO)), ("part", (2, NO)), ("got", (NO, 1), 2), ("got", (NO, 1), 3),
    ("own", 3), ("end", (NO, 2)), ("own", (NO, 1)), ("peer", 3), ("part", 3), ("part", (1, NO)),
    ("peer", (NO, 1)), ("part", (NO, 1)), ("part", 0), ("end", (2, NO)),
    ("end", 3), ("loss", 0), ("done", (2,)), ("end", 1), ("end", 0),
    ("drain", 0), ("done", (3,)), ("done", (1,)), ("done", (0,)),
)
PLAN_ONE = tuple(
    (op, (0,) if op == "done" else 0) + ((True,) if op == "send" else ())
    for op in ("send", "load", "got", "route", "weigh", "own", "peer", "part", "end", "loss", "drain", "done")
)


def dot(a, b, dims=((1,), (0,))):
    return lax.dot_general(a, b, (dims, ((), ())), preferred_element_type=F32)


def iota(shape, axis):
    return lax.broadcasted_iota(jnp.int32, shape, axis)


def kernel(
    n, dpn, cap, groups,
    tok_hbm, router_hbm, ids_hbm, gate_hbm, up_hbm, down_hbm,
    mix_ref, z_ref,
    tok_ref, router_ref, ids_ref, snd, rx, px, fin, ret, own, ffn_ref, zsnd, zrx, zmid, zdp,
    d_send, d_recv, f_send, f_recv, p_send, p_recv, r_send, r_recv,
    z_send, z_recv, y_send, y_recv, w_sem, i_sem,
    hi_ref, lo_ref, w_ref, acc_ref, zout, o_sem,
):
    rows, width = tok_hbm.shape
    topk = ids_hbm.shape[0]
    size = n // groups
    mains = cap // TILE
    rest = cap - mains * TILE
    slot = 1
    while slot < rest:
        slot *= 2
    cuts = TILE // slot
    part = width // cuts
    base = mains * width
    me = lax.axis_index("expert")
    dp = lax.axis_index("dp")
    zone = me // size
    lane = me % size

    plan = PLAN if groups == 4 else PLAN_ONE
    inner = ((zone + 1) // 2) % 2 if groups == 4 else 0
    tail = [step[1] for step in plan if step[0] == "done"]

    def home(k):
        return isinstance(k, int) and k == 0

    def zone_of(k):
        if groups == 4:
            return ((zone // 2 + k // 2) % 2) * 2 + (zone % 2 + k % 2) % 2
        return (zone + k) % groups

    def peer_of(j):
        return (dp + j) % dpn

    def landed(ref, sem):
        pltpu.make_async_copy(ref, ref, sem).wait()

    inputs = [
        pltpu.make_async_copy(src, dst, i_sem.at[i])
        for i, (src, dst) in enumerate(
            ((ids_hbm, ids_ref), (tok_hbm, tok_ref), (router_hbm, router_ref))
        )
    ]
    for load in inputs:
        load.start()
    for i, src in enumerate((gate_hbm, up_hbm, down_hbm)):
        pltpu.make_async_copy(src.at[0], ffn_ref.at[i], w_sem).start()

    z_copy = pltpu.make_async_copy(zout, z_ref, o_sem)
    barrier = pltpu.get_barrier_semaphore()

    def greet(j, c):
        pl.semaphore_signal(
            barrier, inc=1, device_id={"expert": (me + j) % n}, device_id_type=MESH
        )
        return c

    lax.fori_loop(1, n, greet, 0)
    for j in range(1, dpn):
        pl.semaphore_signal(
            barrier, inc=1, device_id={"dp": peer_of(j)}, device_id_type=MESH
        )

    inputs[0].wait()
    hot_t = [(ids_ref[k : k + 1, :] == iota((n, rows), 0)) for k in range(topk)]
    all_t = sum(h.astype(F32) for h in hot_t).astype(BF16)
    upper = (iota((rows, rows), 0) < iota((rows, rows), 1)).astype(F32).astype(BF16)
    before_t = dot(all_t, upper)
    pos_t = [
        jnp.sum(jnp.where(h, before_t, 0.0), axis=0, keepdims=True).astype(jnp.int32)
        for h in hot_t
    ]

    def targets(ids, pos):
        out = []
        for m in range(mains):
            inside = (pos >= m * TILE) & (pos < (m + 1) * TILE)
            out.append(jnp.where(inside, ids * TILE + pos - m * TILE, -1))
        for c in range(cuts if rest else 0):
            inside = pos >= mains * TILE
            out.append(jnp.where(inside, ids * TILE + c * slot + pos - mains * TILE, -1))
        return out

    inputs[1].wait()
    inputs[2].wait()
    goal_t = [targets(ids_ref[k : k + 1, :], pos_t[k]) for k in range(topk)]
    row_at = iota((size * TILE, rows), 0)

    def dispatch(to, at):
        return pltpu.make_async_remote_copy(
            src_ref=snd.at[to], dst_ref=rx.at[dp, at],
            send_sem=d_send, recv_sem=d_recv.at[at],
            device_id={"expert": to}, device_id_type=MESH,
        )

    def forward(j, at, whose):
        return pltpu.make_async_remote_copy(
            src_ref=rx.at[dp, at], dst_ref=rx.at[whose, at],
            send_sem=f_send, recv_sem=f_recv.at[dpn - 1 - j, at // size],
            device_id={"dp": peer_of(j)}, device_id_type=MESH,
        )

    def send_group(k, entry=False):
        first = zone_of(k) * size
        mine = pl.ds(first, size)

        def pick(i):
            at = row_at + first * TILE
            hit = at == goal_t[0][i]
            for c in range(1, topk):
                hit = hit | (at == goal_t[c][i])
            return hit.astype(F32).astype(BF16)

        for m in range(mains):
            snd[mine, :, m * width : (m + 1) * width] = (
                dot(pick(m), tok_ref[...]).astype(BF16).reshape(size, TILE, width)
            )
        if rest:
            extra = sum(
                dot(pick(mains + c), tok_ref[:, c * part : (c + 1) * part])
                for c in range(cuts)
            )
            snd[mine, :, base:] = extra.astype(BF16).reshape(size, TILE, part)
        if entry:
            pl.semaphore_wait(barrier, n - 1 + dpn - 1)

        def one(j, c):
            to = first + (lane + j) % size
            dispatch(to, me).start()
            return c

        lax.fori_loop(1 if home(k) else 0, size, one, 0)
        if home(k):
            rx[dp, me] = snd[me]
            for q in range(1, dpn):
                forward(q, me, dp).start()

    count = size * TILE
    at_row, at_col = iota((count, count), 0), iota((count, count), 1)
    per_cut = size * slot
    want = ((at_row % per_cut) // slot) * TILE + (at_row // per_cut) * slot + at_row % slot
    order = (at_col == want).astype(F32).astype(BF16)

    def natural(block):
        pieces = [
            block[:, :, m * width : (m + 1) * width].reshape(count, width)
            for m in range(mains)
        ]
        if rest:
            sorted_rows = dot(order, block[:, :, base:].reshape(count, part)).astype(BF16)
            pieces.append(
                jnp.concatenate(
                    [sorted_rows[c * per_cut : (c + 1) * per_cut] for c in range(cuts)],
                    axis=1,
                )
            )
        return pieces

    def blocks_of(rows_out, store):
        for m in range(mains):
            store(
                m * width, width,
                rows_out[m * count : (m + 1) * count].reshape(size, TILE, width),
            )
        if rest:
            tail = rows_out[mains * count :]
            stacked = jnp.concatenate(
                [tail[:, c * part : (c + 1) * part] for c in range(cuts)], axis=0
            )
            mixed = dot(order, stacked, ((0,), (0,))).astype(BF16)
            store(base, part, mixed.reshape(size, TILE, part))

    def expert(block):
        x = jnp.concatenate(natural(block), axis=0)
        gate = dot(x, ffn_ref[0], ((1,), (1,)))
        up = dot(x, ffn_ref[1], ((1,), (1,)))
        hidden = (gate / (1.0 + jnp.exp(-gate)) * up).astype(BF16)
        return dot(hidden, ffn_ref[2])

    def partial_copy(j, t, half):
        if half is None:
            mine = pl.ds(zone_of(t) * size, size)
        else:
            mine = pl.ds(zone_of(t) * size + half * (size // 2), size // 2)
        return pltpu.make_async_remote_copy(
            src_ref=rx.at[peer_of(j), mine], dst_ref=px.at[dp, mine],
            send_sem=p_send, recv_sem=p_recv.at[dpn - 1 - j, zone_of(t)],
            device_id={"dp": peer_of(j)}, device_id_type=MESH,
        )

    def give_back(to, at):
        return pltpu.make_async_remote_copy(
            src_ref=fin.at[to], dst_ref=ret.at[at],
            send_sem=r_send, recv_sem=r_recv.at[at // size],
            device_id={"expert": to}, device_id_type=MESH,
        )

    def loss_copy(to, at):
        return pltpu.make_async_remote_copy(
            src_ref=zsnd, dst_ref=zrx.at[at],
            send_sem=z_send, recv_sem=z_recv,
            device_id={"expert": to}, device_id_type=MESH,
        )

    def loss_dp(j, whose):
        return pltpu.make_async_remote_copy(
            src_ref=zmid, dst_ref=zdp.at[whose],
            send_sem=y_send, recv_sem=y_recv,
            device_id={"dp": peer_of(j)}, device_id_type=MESH,
        )

    def route():
        logits = dot(tok_ref[...], router_ref[...], ((1,), (1,)))
        top = jnp.max(logits, axis=1, keepdims=True)
        log_total = top + jnp.log(jnp.sum(jnp.exp(logits - top), axis=1, keepdims=True))
        local = jnp.sum(log_total * log_total, axis=0, keepdims=True)
        zsnd[...] = jnp.broadcast_to(local, zsnd.shape)
        zrx[me] = jnp.broadcast_to(local, zsnd.shape)

        def send_loss(j, c):
            loss_copy((me + j) % n, me).start()
            return c

        lax.fori_loop(1, n, send_loss, 0)

        same = (iota((n, n), 0) == iota((n, n), 1)).astype(F32).astype(BF16)
        hot = [dot(h.astype(F32).astype(BF16), same, ((0,), (0,))) > 0.5 for h in hot_t]
        ids = [
            jnp.sum(jnp.where(h, iota((rows, n), 1), 0), axis=1, keepdims=True) for h in hot
        ]
        chosen = [jnp.sum(jnp.where(h, logits, 0.0), axis=1, keepdims=True) for h in hot]
        high = functools.reduce(jnp.maximum, chosen)
        exps = [jnp.exp(c - high) for c in chosen]
        share = [e / sum(exps) for e in exps]
        all_hot = sum(h.astype(F32) for h in hot).astype(BF16)
        lower = (iota((rows, rows), 1) < iota((rows, rows), 0)).astype(F32).astype(BF16)
        before = dot(lower, all_hot)
        pos = [
            jnp.sum(jnp.where(h, before, 0.0), axis=1, keepdims=True).astype(jnp.int32)
            for h in hot
        ]
        goal = [targets(ids[k], pos[k]) for k in range(topk)]

        col_at = iota((rows, n * TILE), 1)
        for i in range(mains + (cuts if rest else 0)):
            w = sum(jnp.where(col_at == goal[k][i], share[k], 0.0) for k in range(topk))
            hi = w.astype(BF16)
            hi_ref[i] = hi
            lo_ref[i] = (w - hi.astype(F32)).astype(BF16)

    def arrive(k, part=None):
        first = zone_of(k) * size

        def one(j, c):
            at = first + (lane + size - j) % size
            dispatch(at, at).wait_recv()
            for q in range(1, dpn):
                forward(q, at, dp).start()
            return c

        if part is None:
            lax.fori_loop(1 if home(k) else 0, size, one, 0)
        else:
            quarter = size // 4
            lax.fori_loop(part * quarter, (part + 1) * quarter, one, 0)

    def own_part(k):
        own[k] = expert(rx[dp, pl.ds(zone_of(k) * size, size)])

    def peer_part(k):
        first = zone_of(k) * size

        def one(q, c):
            whose = peer_of(q)

            landed(rx.at[whose, pl.ds(first, size)], f_recv.at[q - 1, zone_of(k)])
            out = expert(rx[whose, pl.ds(first, size)]).astype(BF16)

            def store(start, wide, value):
                rx[whose, pl.ds(first, size), :, start : start + wide] = value

            blocks_of(out, store)
            return c

        lax.fori_loop(1, dpn, one, 0)

    def send_part(k, half=None):
        for q in range(1, dpn):
            partial_copy(q, k, half).start()

    def finish(k):
        first = zone_of(k) * size
        total = own[k]
        for q in range(1, dpn):
            landed(px.at[peer_of(q), pl.ds(first, size)], p_recv.at[q - 1, zone_of(k)])
            block = px[peer_of(q), pl.ds(first, size)]
            total = total + jnp.concatenate(natural(block), axis=0).astype(F32)

        def store(start, wide, value):
            fin[pl.ds(first, size), :, start : start + wide] = value

        blocks_of(total.astype(BF16), store)

        def back(j, c):
            give_back(first + (lane + j) % size, me).start()
            return c

        lax.fori_loop(1 if home(k) else 0, size, back, 0)
        if home(k):
            ret[me] = fin[me]

    def cut(i, k):
        start = zone_of(k) * size * TILE
        sub = (iota((n * TILE, size * TILE), 0) == iota((n * TILE, size * TILE), 1) + start)
        sub = sub.astype(F32).astype(BF16)
        hi = dot(hi_ref[i], sub).astype(BF16)
        lo = dot(lo_ref[i], sub).astype(BF16)
        return jnp.concatenate([hi, lo], axis=1)

    def weigh(k):
        for i in range(mains + (cuts if rest else 0)):
            for k in range(groups):
                w_ref[i, k] = cut(i, k)

    def take(ks):
        for k in ks:
            here = pl.ds(zone_of(k) * size, size - 1 if home(k) else size)
            landed(ret.at[here], r_recv.at[zone_of(k)])

        def twice(x):
            return jnp.concatenate([x, x], axis=0)

        for c in range(cuts):
            cols = slice(c * part, (c + 1) * part)
            acc = 0.0 if ks == tail[0] else acc_ref[:, cols]
            for k in ks:
                mine = pl.ds(zone_of(k) * size, size)
                for m in range(mains):
                    seen = ret[mine, :, m * width + c * part : m * width + (c + 1) * part]
                    acc = acc + dot(w_ref[m, k], twice(seen.reshape(count, part)))
                if rest:
                    seen = ret[mine, :, base:].reshape(count, part)
                    acc = acc + dot(w_ref[mains + c, k], twice(seen))
            if ks == tail[-1]:
                mix_ref[:, cols] = acc.astype(BF16)
            else:
                acc_ref[:, cols] = acc

    def loads_in(k):
        landed(ffn_ref, w_sem)

    def gather_loss():
        landed(zrx.at[pl.ds(0, n - 1)], z_recv)
        mid = zrx[0]
        for i in range(1, n):
            mid = mid + zrx[i]
        zmid[...] = mid
        zdp[dp] = mid

        for q in range(1, dpn):
            loss_dp(q, dp).start()

    def drain(k):
        landed(snd.at[pl.ds(0, n - 1)], d_send)
        landed(zrx.at[pl.ds(0, n - 1)], z_send)
        landed(rx.at[pl.ds(0, dpn - 1)], f_send)
        landed(px.at[pl.ds(0, dpn - 1)], p_send)
        landed(zdp.at[pl.ds(0, dpn - 1)], y_send)
        landed(zdp.at[pl.ds(0, dpn - 1)], y_recv)
        loss = zdp[dp]
        for q in range(1, dpn):
            loss = loss + zdp[peer_of(q)]
        zout[...] = loss[0:1, 0:1] / F32(rows * n * dpn)
        z_copy.start()

    steps = {
        "send": send_group, "got": arrive, "own": own_part, "peer": peer_part,
        "part": send_part, "end": finish, "done": take, "load": loads_in,
        "route": lambda k: route(), "loss": lambda k: gather_loss(), "weigh": weigh, "drain": drain,
    }
    for op, at, *more in plan:
        with jax.named_scope(f"{op}_{at}_{more}"):
            if op == "done" or not isinstance(at, tuple):
                steps[op](at, *more)
            elif None in at:
                chosen = at[0] if at[1] is None else at[1]
                pl.when(inner == at.index(chosen))(functools.partial(steps[op], chosen, *more))
            else:
                steps[op](at[0] + inner * (at[1] - at[0]), *more)

    z_copy.wait()

    landed(fin.at[pl.ds(0, n - 1)], r_send)


def on_device(n, dpn, tokens, router_weight, route_ids, gate_weight, up_weight, down_weight):
    rows, width = tokens.shape
    topk = route_ids.shape[1]
    experts = router_weight.shape[1]
    assert experts == n and gate_weight.shape[0] == 1
    cap = 5 * rows * topk // (4 * experts)
    groups = 4 if n % 4 == 0 else 1
    mains, rest = cap // TILE, cap % TILE
    slot = 1
    while slot < rest:
        slot *= 2
    block = mains * width + (width * slot // TILE if rest else 0)
    size = n // groups
    in_rows = size * TILE * mains + (size * slot if rest else 0)
    hidden = gate_weight.shape[1]
    vmem = pl.BlockSpec(memory_space=pltpu.VMEM)
    hbm = pl.BlockSpec(memory_space=pl.ANY)
    dma = pltpu.SemaphoreType.DMA
    mixture, loss = pl.pallas_call(
        functools.partial(kernel, n, dpn, cap, groups),
        out_shape=(
            pltpu.VMEM((rows, width), BF16),
            jax.ShapeDtypeStruct((1, 1), F32),
        ),
        in_specs=[hbm] * 6,
        out_specs=(vmem, hbm),
        scratch_shapes=[
            pltpu.VMEM((rows, width), BF16),
            pltpu.VMEM((experts, width), BF16),
            pltpu.VMEM((topk, rows), jnp.int32),
            pltpu.VMEM((n, TILE, block), BF16),
            pltpu.VMEM((dpn, n, TILE, block), BF16),
            pltpu.VMEM((dpn, n, TILE, block), BF16),
            pltpu.VMEM((n, TILE, block), BF16),
            pltpu.VMEM((n, TILE, block), BF16),
            pltpu.VMEM((groups, in_rows, width), F32),
            pltpu.VMEM((3, hidden, width), BF16),
            pltpu.VMEM((8, 128), F32),
            pltpu.VMEM((n, 8, 128), F32),
            pltpu.VMEM((8, 128), F32),
            pltpu.VMEM((dpn, 8, 128), F32),
            dma, dma((n,)), dma, dma((dpn - 1, groups)),
            dma, dma((dpn - 1, groups)), dma, dma((groups,)),
            dma, dma, dma, dma, dma, dma((3,)),
            pltpu.VMEM((mains + (TILE // slot if rest else 0), rows, n * TILE), BF16),
            pltpu.VMEM((mains + (TILE // slot if rest else 0), rows, n * TILE), BF16),
            pltpu.VMEM((mains + (TILE // slot if rest else 0), groups, rows, 2 * size * TILE), BF16),
            pltpu.VMEM((rows, width), F32),
            pltpu.VMEM((1, 1), F32),
            dma,
        ],
        compiler_params=pltpu.CompilerParams(
            collective_id=0, has_side_effects=True, vmem_limit_bytes=60 * 1024 * 1024
        ),
    )(tokens, router_weight.T, route_ids.T, gate_weight, up_weight, down_weight)
    return mixture, loss[0, 0]


def solution(mesh):
    in_specs = (
        P(("dp", "expert"), None),
        P(),
        P(("dp", "expert"), None),
        P("expert", "dp", None),
        P("expert", "dp", None),
        P("expert", "dp", None),
    )
    out_specs = (P(("dp", "expert"), None), P())
    return jax.shard_map(
        functools.partial(on_device, mesh.shape["expert"], mesh.shape["dp"]),
        mesh=mesh, in_specs=in_specs, out_specs=out_specs, check_vma=False,
    )
```

```python
import functools

import jax
import jax.numpy as jnp
from jax import lax
from jax.experimental import pallas as pl
from jax.experimental.pallas import tpu as pltpu
from jax.sharding import PartitionSpec as P

MESH = pl.DeviceIdType.MESH
F32 = jnp.float32
BF16 = jnp.bfloat16
TILE = 16
NO = None
PLAN = (
    ("send", (2, 1), True), ("send", 0), ("send", (1, 2)), ("send", 3),
    ("load", 0), ("got", 0), ("own", 0),
    ("got", (1, 2), 0), ("got", (1, 2), 1), ("route", 0), ("got", (1, 2), 2), ("got", (1, 2), 3),
    ("own", (1, 2)), ("peer", 0),
    ("got", (2, 1), 0), ("got", (2, 1), 1),
    ("weigh", 0), ("peer", (1, 2)), ("part", (NO, 2), 0), ("part", (NO, 2), 1),
    ("got", (2, 1), 2), ("got", (2, 1), 3), ("own", (2, 1)),
    ("got", 3, 0), ("got", 3, 1), ("got", 3, 2), ("got", 3, 3),
    ("peer", (2, NO)), ("part", (2, NO), 0), ("part", (2, NO), 1),
    ("own", 3), ("end", (NO, 2), 0), ("end", (NO, 2), 1),
    ("peer", (NO, 1)), ("part", (NO, 1), 0), ("part", (NO, 1), 1),
    ("peer", 3), ("part", 3, 0), ("part", 3, 1), ("part", (1, NO), 0), ("part", (1, NO), 1),
    ("part", 0, 0), ("part", 0, 1),
    ("end", (2, 1), 0), ("end", (2, 1), 1), ("end", 3, 0), ("end", 3, 1), ("loss", 0),
    ("end", (1, NO), 0), ("end", (1, NO), 1), ("end", 0, 0), ("done", (2,)), ("end", 0, 1),
    ("drain", 0), ("done", (1,)), ("done", (3,)), ("done", (0,)),
)
PLAN_ONE = tuple(
    (op, (0,) if op == "done" else 0) + ((True,) if op == "send" else ())
    for op in ("send", "load", "got", "route", "weigh", "own", "peer", "part", "end", "loss", "drain", "done")
)


def dot(a, b, dims=((1,), (0,))):
    return lax.dot_general(a, b, (dims, ((), ())), preferred_element_type=F32)


def iota(shape, axis):
    return lax.broadcasted_iota(jnp.int32, shape, axis)


def kernel(
    n, dpn, cap, groups,
    tok_hbm, router_hbm, ids_hbm, gate_hbm, up_hbm, down_hbm,
    mix_ref, z_ref,
    tok_ref, router_ref, ids_ref, snd, rx, px, fin, ret, own, ffn_ref, zsnd, zrx, zmid, zdp,
    d_send, d_recv, f_send, f_recv, p_send, p_recv, r_send, r_recv,
    z_send, z_recv, y_send, y_recv, w_sem, i_sem,
    hi_ref, lo_ref, w_ref, acc_ref, zout, o_sem,
):
    rows, width = tok_hbm.shape
    topk = ids_hbm.shape[0]
    size = n // groups
    mains = cap // TILE
    rest = cap - mains * TILE
    slot = 1
    while slot < rest:
        slot *= 2
    cuts = TILE // slot
    part = width // cuts
    base = mains * width
    me = lax.axis_index("expert")
    dp = lax.axis_index("dp")
    zone = me // size
    lane = me % size

    plan = PLAN if groups == 4 else PLAN_ONE
    inner = ((zone + 1) // 2) % 2 if groups == 4 else 0
    tail = [step[1] for step in plan if step[0] == "done"]

    def home(k):
        return isinstance(k, int) and k == 0

    def zone_of(k):
        if groups == 4:
            return ((zone // 2 + k // 2) % 2) * 2 + (zone % 2 + k % 2) % 2
        return (zone + k) % groups

    def peer_of(j):
        return (dp + j) % dpn

    def landed(ref, sem):
        pltpu.make_async_copy(ref, ref, sem).wait()

    inputs = [
        pltpu.make_async_copy(src, dst, i_sem.at[i])
        for i, (src, dst) in enumerate(
            ((ids_hbm, ids_ref), (tok_hbm, tok_ref), (router_hbm, router_ref))
        )
    ]
    for load in inputs:
        load.start()
    for i, src in enumerate((gate_hbm, up_hbm, down_hbm)):
        pltpu.make_async_copy(src.at[0], ffn_ref.at[i], w_sem).start()

    z_copy = pltpu.make_async_copy(zout, z_ref, o_sem)
    barrier = pltpu.get_barrier_semaphore()

    def greet(j, c):
        pl.semaphore_signal(
            barrier, inc=1, device_id={"expert": (me + j) % n}, device_id_type=MESH
        )
        return c

    lax.fori_loop(1, n, greet, 0)
    for j in range(1, dpn):
        pl.semaphore_signal(
            barrier, inc=1, device_id={"dp": peer_of(j)}, device_id_type=MESH
        )

    inputs[0].wait()
    hot_t = [(ids_ref[k : k + 1, :] == iota((n, rows), 0)) for k in range(topk)]
    all_t = sum(h.astype(F32) for h in hot_t).astype(BF16)
    upper = (iota((rows, rows), 0) < iota((rows, rows), 1)).astype(F32).astype(BF16)
    before_t = dot(all_t, upper)
    pos_t = [
        jnp.sum(jnp.where(h, before_t, 0.0), axis=0, keepdims=True).astype(jnp.int32)
        for h in hot_t
    ]

    def targets(ids, pos):
        out = []
        for m in range(mains):
            inside = (pos >= m * TILE) & (pos < (m + 1) * TILE)
            out.append(jnp.where(inside, ids * TILE + pos - m * TILE, -1))
        for c in range(cuts if rest else 0):
            inside = pos >= mains * TILE
            out.append(jnp.where(inside, ids * TILE + c * slot + pos - mains * TILE, -1))
        return out

    inputs[1].wait()
    inputs[2].wait()
    goal_t = [targets(ids_ref[k : k + 1, :], pos_t[k]) for k in range(topk)]
    row_at = iota((size * TILE, rows), 0)

    def dispatch(to, at):
        return pltpu.make_async_remote_copy(
            src_ref=snd.at[to], dst_ref=rx.at[dp, at],
            send_sem=d_send, recv_sem=d_recv.at[at],
            device_id={"expert": to}, device_id_type=MESH,
        )

    def forward(j, at, whose):
        return pltpu.make_async_remote_copy(
            src_ref=rx.at[dp, at], dst_ref=rx.at[whose, at],
            send_sem=f_send, recv_sem=f_recv.at[dpn - 1 - j, at // size],
            device_id={"dp": peer_of(j)}, device_id_type=MESH,
        )

    def send_group(k, entry=False):
        first = zone_of(k) * size
        mine = pl.ds(first, size)

        def pick(i):
            at = row_at + first * TILE
            hit = at == goal_t[0][i]
            for c in range(1, topk):
                hit = hit | (at == goal_t[c][i])
            return hit.astype(F32).astype(BF16)

        for m in range(mains):
            snd[mine, :, m * width : (m + 1) * width] = (
                dot(pick(m), tok_ref[...]).astype(BF16).reshape(size, TILE, width)
            )
        if rest:
            extra = sum(
                dot(pick(mains + c), tok_ref[:, c * part : (c + 1) * part])
                for c in range(cuts)
            )
            snd[mine, :, base:] = extra.astype(BF16).reshape(size, TILE, part)
        if entry:
            pl.semaphore_wait(barrier, n - 1 + dpn - 1)

        def one(j, c):
            to = first + (lane + j) % size
            dispatch(to, me).start()
            return c

        lax.fori_loop(1 if home(k) else 0, size, one, 0)
        if home(k):
            rx[dp, me] = snd[me]
            for q in range(1, dpn):
                forward(q, me, dp).start()

    def order_of(blocks):
        full = blocks * TILE
        at_row, at_col = iota((full, full), 0), iota((full, full), 1)
        per_cut = blocks * slot
        want = ((at_row % per_cut) // slot) * TILE + (at_row // per_cut) * slot + at_row % slot
        return (at_col == want).astype(F32).astype(BF16)

    def part_of(k, half):
        if half is None:
            return zone_of(k) * size, size, 0
        near = lane // (size // 2)
        side = near if half else (near + 1) % 2
        return zone_of(k) * size + side * (size // 2), size // 2, side

    count = size * TILE

    def natural(block):
        blocks = block.shape[0]
        count, per_cut, order = blocks * TILE, blocks * slot, order_of(blocks)
        pieces = [
            block[:, :, m * width : (m + 1) * width].reshape(count, width)
            for m in range(mains)
        ]
        if rest:
            sorted_rows = dot(order, block[:, :, base:].reshape(count, part)).astype(BF16)
            pieces.append(
                jnp.concatenate(
                    [sorted_rows[c * per_cut : (c + 1) * per_cut] for c in range(cuts)],
                    axis=1,
                )
            )
        return pieces

    def blocks_of(rows_out, blocks, store):
        count, order = blocks * TILE, order_of(blocks)
        for m in range(mains):
            store(
                m * width, width,
                rows_out[m * count : (m + 1) * count].reshape(blocks, TILE, width),
            )
        if rest:
            extra = rows_out[mains * count :]
            stacked = jnp.concatenate(
                [extra[:, c * part : (c + 1) * part] for c in range(cuts)], axis=0
            )
            mixed = dot(order, stacked, ((0,), (0,))).astype(BF16)
            store(base, part, mixed.reshape(blocks, TILE, part))

    def expert(block):
        x = jnp.concatenate(natural(block), axis=0)
        gate = dot(x, ffn_ref[0], ((1,), (1,)))
        up = dot(x, ffn_ref[1], ((1,), (1,)))
        hidden = (gate / (1.0 + jnp.exp(-gate)) * up).astype(BF16)
        return dot(hidden, ffn_ref[2])

    def partial_copy(j, t, half):
        first, blocks, _ = part_of(t, half)
        mine = pl.ds(first, blocks)
        return pltpu.make_async_remote_copy(
            src_ref=rx.at[peer_of(j), mine], dst_ref=px.at[dp, mine],
            send_sem=p_send, recv_sem=p_recv.at[dpn - 1 - j, zone_of(t), half or 0],
            device_id={"dp": peer_of(j)}, device_id_type=MESH,
        )

    def give_back(to, at):
        return pltpu.make_async_remote_copy(
            src_ref=fin.at[to], dst_ref=ret.at[at],
            send_sem=r_send, recv_sem=r_recv.at[at // size],
            device_id={"expert": to}, device_id_type=MESH,
        )

    def loss_copy(to, at):
        return pltpu.make_async_remote_copy(
            src_ref=zsnd, dst_ref=zrx.at[at],
            send_sem=z_send, recv_sem=z_recv,
            device_id={"expert": to}, device_id_type=MESH,
        )

    def loss_dp(j, whose):
        return pltpu.make_async_remote_copy(
            src_ref=zmid, dst_ref=zdp.at[whose],
            send_sem=y_send, recv_sem=y_recv,
            device_id={"dp": peer_of(j)}, device_id_type=MESH,
        )

    def route():
        logits = dot(tok_ref[...], router_ref[...], ((1,), (1,)))
        top = jnp.max(logits, axis=1, keepdims=True)
        log_total = top + jnp.log(jnp.sum(jnp.exp(logits - top), axis=1, keepdims=True))
        local = jnp.sum(log_total * log_total, axis=0, keepdims=True)
        zsnd[...] = jnp.broadcast_to(local, zsnd.shape)
        zrx[me] = jnp.broadcast_to(local, zsnd.shape)

        def send_loss(j, c):
            loss_copy((me + j) % n, me).start()
            return c

        lax.fori_loop(1, n, send_loss, 0)

        same = (iota((n, n), 0) == iota((n, n), 1)).astype(F32).astype(BF16)
        hot = [dot(h.astype(F32).astype(BF16), same, ((0,), (0,))) > 0.5 for h in hot_t]
        ids = [
            jnp.sum(jnp.where(h, iota((rows, n), 1), 0), axis=1, keepdims=True) for h in hot
        ]
        chosen = [jnp.sum(jnp.where(h, logits, 0.0), axis=1, keepdims=True) for h in hot]
        high = functools.reduce(jnp.maximum, chosen)
        exps = [jnp.exp(c - high) for c in chosen]
        share = [e / sum(exps) for e in exps]
        all_hot = sum(h.astype(F32) for h in hot).astype(BF16)
        lower = (iota((rows, rows), 1) < iota((rows, rows), 0)).astype(F32).astype(BF16)
        before = dot(lower, all_hot)
        pos = [
            jnp.sum(jnp.where(h, before, 0.0), axis=1, keepdims=True).astype(jnp.int32)
            for h in hot
        ]
        goal = [targets(ids[k], pos[k]) for k in range(topk)]

        col_at = iota((rows, n * TILE), 1)
        for i in range(mains + (cuts if rest else 0)):
            w = sum(jnp.where(col_at == goal[k][i], share[k], 0.0) for k in range(topk))
            hi = w.astype(BF16)
            hi_ref[i] = hi
            lo_ref[i] = (w - hi.astype(F32)).astype(BF16)

    def arrive(k, part=None):
        first = zone_of(k) * size

        def one(j, c):
            at = first + (lane + size - j) % size
            dispatch(at, at).wait_recv()
            for q in range(1, dpn):
                forward(q, at, dp).start()
            return c

        if part is None:
            lax.fori_loop(1 if home(k) else 0, size, one, 0)
        else:
            quarter = size // 4
            lax.fori_loop(part * quarter, (part + 1) * quarter, one, 0)

    def own_part(k):
        own[k] = expert(rx[dp, pl.ds(zone_of(k) * size, size)])

    def peer_part(k):
        first = zone_of(k) * size

        def one(q, c):
            whose = peer_of(q)

            landed(rx.at[whose, pl.ds(first, size)], f_recv.at[q - 1, zone_of(k)])
            out = expert(rx[whose, pl.ds(first, size)]).astype(BF16)

            def store(start, wide, value):
                rx[whose, pl.ds(first, size), :, start : start + wide] = value

            blocks_of(out, size, store)
            return c

        lax.fori_loop(1, dpn, one, 0)

    def send_part(k, half=None):
        for q in range(1, dpn):
            partial_copy(q, k, half).start()

    def finish(k, half=None):
        first, blocks, side = part_of(k, half)
        if half is None:
            total = own[k]
        else:
            total = []
            for at, tall in [(m * count, blocks * TILE) for m in range(mains)] + (
                [(mains * count, blocks * slot)] if rest else []
            ):
                total.append(own[k, pl.ds(pl.multiple_of(at + side * tall, 8), tall), :])
            total = jnp.concatenate(total, axis=0)
        for q in range(1, dpn):
            block = px.at[peer_of(q), pl.ds(first, blocks)]
            landed(block, p_recv.at[q - 1, zone_of(k), half or 0])
            total = total + jnp.concatenate(natural(block[...]), axis=0).astype(F32)

        def store(start, wide, value):
            fin[pl.ds(first, blocks), :, start : start + wide] = value

        blocks_of(total.astype(BF16), blocks, store)
        mixed = home(k) and half != 0

        def back(j, c):
            give_back(first + (lane % blocks + j) % blocks, me).start()
            return c

        lax.fori_loop(1 if mixed else 0, blocks, back, 0)
        if mixed:
            ret[me] = fin[me]

    def cut(i, k):
        start = zone_of(k) * size * TILE
        sub = (iota((n * TILE, size * TILE), 0) == iota((n * TILE, size * TILE), 1) + start)
        sub = sub.astype(F32).astype(BF16)
        hi = dot(hi_ref[i], sub).astype(BF16)
        lo = dot(lo_ref[i], sub).astype(BF16)
        return jnp.concatenate([hi, lo], axis=1)

    def weigh(k):
        for i in range(mains + (cuts if rest else 0)):
            for k in range(groups):
                w_ref[i, k] = cut(i, k)

    def take(ks):
        for k in ks:
            here = pl.ds(zone_of(k) * size, size - 1 if home(k) else size)
            landed(ret.at[here], r_recv.at[zone_of(k)])

        def twice(x):
            return jnp.concatenate([x, x], axis=0)

        for c in range(cuts):
            cols = slice(c * part, (c + 1) * part)
            acc = 0.0 if ks == tail[0] else acc_ref[:, cols]
            for k in ks:
                mine = pl.ds(zone_of(k) * size, size)
                for m in range(mains):
                    seen = ret[mine, :, m * width + c * part : m * width + (c + 1) * part]
                    acc = acc + dot(w_ref[m, k], twice(seen.reshape(count, part)))
                if rest:
                    seen = ret[mine, :, base:].reshape(count, part)
                    acc = acc + dot(w_ref[mains + c, k], twice(seen))
            if ks == tail[-1]:
                mix_ref[:, cols] = acc.astype(BF16)
            else:
                acc_ref[:, cols] = acc

    def loads_in(k):
        landed(ffn_ref, w_sem)

    def gather_loss():
        landed(zrx.at[pl.ds(0, n - 1)], z_recv)
        mid = zrx[0]
        for i in range(1, n):
            mid = mid + zrx[i]
        zmid[...] = mid
        zdp[dp] = mid

        for q in range(1, dpn):
            loss_dp(q, dp).start()

    def drain(k):
        landed(snd.at[pl.ds(0, n - 1)], d_send)
        landed(zrx.at[pl.ds(0, n - 1)], z_send)
        landed(rx.at[pl.ds(0, dpn - 1)], f_send)
        landed(px.at[pl.ds(0, dpn - 1)], p_send)
        landed(zdp.at[pl.ds(0, dpn - 1)], y_send)
        landed(zdp.at[pl.ds(0, dpn - 1)], y_recv)
        loss = zdp[dp]
        for q in range(1, dpn):
            loss = loss + zdp[peer_of(q)]
        zout[...] = loss[0:1, 0:1] / F32(rows * n * dpn)
        z_copy.start()

    steps = {
        "send": send_group, "got": arrive, "own": own_part, "peer": peer_part,
        "part": send_part, "end": finish, "done": take, "load": loads_in,
        "route": lambda k: route(), "loss": lambda k: gather_loss(), "weigh": weigh, "drain": drain,
    }
    for op, at, *more in plan:
        with jax.named_scope(f"{op}_{at}_{more}"):
            if op == "done" or not isinstance(at, tuple):
                steps[op](at, *more)
            elif None in at:
                chosen = at[0] if at[1] is None else at[1]
                pl.when(inner == at.index(chosen))(functools.partial(steps[op], chosen, *more))
            else:
                steps[op](at[0] + inner * (at[1] - at[0]), *more)

    z_copy.wait()

    landed(fin.at[pl.ds(0, n - 1)], r_send)


def on_device(n, dpn, tokens, router_weight, route_ids, gate_weight, up_weight, down_weight):
    rows, width = tokens.shape
    topk = route_ids.shape[1]
    experts = router_weight.shape[1]
    assert experts == n and gate_weight.shape[0] == 1
    cap = 5 * rows * topk // (4 * experts)
    groups = 4 if n % 4 == 0 else 1
    mains, rest = cap // TILE, cap % TILE
    slot = 1
    while slot < rest:
        slot *= 2
    block = mains * width + (width * slot // TILE if rest else 0)
    size = n // groups
    in_rows = size * TILE * mains + (size * slot if rest else 0)
    hidden = gate_weight.shape[1]
    vmem = pl.BlockSpec(memory_space=pltpu.VMEM)
    hbm = pl.BlockSpec(memory_space=pl.ANY)
    dma = pltpu.SemaphoreType.DMA
    mixture, loss = pl.pallas_call(
        functools.partial(kernel, n, dpn, cap, groups),
        out_shape=(
            pltpu.VMEM((rows, width), BF16),
            jax.ShapeDtypeStruct((1, 1), F32),
        ),
        in_specs=[hbm] * 6,
        out_specs=(vmem, hbm),
        scratch_shapes=[
            pltpu.VMEM((rows, width), BF16),
            pltpu.VMEM((experts, width), BF16),
            pltpu.VMEM((topk, rows), jnp.int32),
            pltpu.VMEM((n, TILE, block), BF16),
            pltpu.VMEM((dpn, n, TILE, block), BF16),
            pltpu.VMEM((dpn, n, TILE, block), BF16),
            pltpu.VMEM((n, TILE, block), BF16),
            pltpu.VMEM((n, TILE, block), BF16),
            pltpu.VMEM((groups, in_rows, width), F32),
            pltpu.VMEM((3, hidden, width), BF16),
            pltpu.VMEM((8, 128), F32),
            pltpu.VMEM((n, 8, 128), F32),
            pltpu.VMEM((8, 128), F32),
            pltpu.VMEM((dpn, 8, 128), F32),
            dma, dma((n,)), dma, dma((dpn - 1, groups)),
            dma, dma((dpn - 1, groups, 2)), dma, dma((groups,)),
            dma, dma, dma, dma, dma, dma((3,)),
            pltpu.VMEM((mains + (TILE // slot if rest else 0), rows, n * TILE), BF16),
            pltpu.VMEM((mains + (TILE // slot if rest else 0), rows, n * TILE), BF16),
            pltpu.VMEM((mains + (TILE // slot if rest else 0), groups, rows, 2 * size * TILE), BF16),
            pltpu.VMEM((rows, width), F32),
            pltpu.VMEM((1, 1), F32),
            dma,
        ],
        compiler_params=pltpu.CompilerParams(
            collective_id=0, has_side_effects=True, vmem_limit_bytes=60 * 1024 * 1024
        ),
    )(tokens, router_weight.T, route_ids.T, gate_weight, up_weight, down_weight)
    return mixture, loss[0, 0]


def solution(mesh):
    in_specs = (
        P(("dp", "expert"), None),
        P(),
        P(("dp", "expert"), None),
        P("expert", "dp", None),
        P("expert", "dp", None),
        P("expert", "dp", None),
    )
    out_specs = (P(("dp", "expert"), None), P())
    return jax.shard_map(
        functools.partial(on_device, mesh.shape["expert"], mesh.shape["dp"]),
        mesh=mesh, in_specs=in_specs, out_specs=out_specs, check_vma=False,
    )
```

```python
import functools

import jax
import jax.numpy as jnp
from jax import lax
from jax.experimental import pallas as pl
from jax.experimental.pallas import tpu as pltpu
from jax.sharding import PartitionSpec as P

MESH = pl.DeviceIdType.MESH
F32 = jnp.float32
BF16 = jnp.bfloat16
TILE = 16
NO = None
PLAN = (
    ("send", (2, 1), True), ("send", 0), ("send", (1, 2)), ("send", 3),
    ("load", 0), ("got", 0), ("own", 0),
    ("got", (1, 2), 0), ("got", (1, 2), 1), ("route", 0), ("got", (1, 2), 2), ("got", (1, 2), 3),
    ("own", (1, 2)), ("peer", 0),
    ("got", (2, 1), 0), ("got", (2, 1), 1),
    ("weigh", 0), ("peer", (1, 2)), ("part", (NO, 2), 0), ("part", (NO, 2), 1),
    ("got", (2, 1), 2), ("got", (2, 1), 3), ("own", (2, 1)),
    ("got", 3, 0), ("got", 3, 1), ("end", (NO, 2), 0), ("got", 3, 2), ("end", (NO, 2), 1), ("got", 3, 3),
    ("peer", (2, NO)), ("part", (2, NO), 0), ("part", (2, NO), 1),
    ("own", 3),
    ("peer", (NO, 1)), ("part", (NO, 1), 0), ("part", (NO, 1), 1),
    ("peer", 3), ("part", 3, 0), ("part", 3, 1), ("part", (1, NO), 0), ("part", 0, 0), ("part", (1, NO), 1),
    ("part", 0, 1),
    ("end", (2, 1), 0), ("end", (2, 1), 1), ("end", 3, 0), ("end", 3, 1), ("loss", 0),
    ("end", (1, NO), 0), ("end", 0, 0), ("end", (1, NO), 1), ("done", (2,)), ("end", 0, 1),
    ("drain", 0), ("done", (1,)), ("done", (3,)), ("done", (0,)),
)
PLAN_ONE = tuple(
    (op, (0,) if op == "done" else 0) + ((True,) if op == "send" else ())
    for op in ("send", "load", "got", "route", "weigh", "own", "peer", "part", "end", "loss", "drain", "done")
)


def dot(a, b, dims=((1,), (0,))):
    return lax.dot_general(a, b, (dims, ((), ())), preferred_element_type=F32)


def iota(shape, axis):
    return lax.broadcasted_iota(jnp.int32, shape, axis)


def kernel(
    n, dpn, cap, groups,
    tok_hbm, router_hbm, ids_hbm, gate_hbm, up_hbm, down_hbm,
    mix_ref, z_ref,
    tok_ref, router_ref, ids_ref, snd, rx, px, fin, ret, own, ffn_ref, zsnd, zrx, zmid, zdp,
    d_send, d_recv, f_send, f_recv, p_send, p_recv, r_send, r_recv,
    z_send, z_recv, y_send, y_recv, w_sem, i_sem,
    hi_ref, lo_ref, w_ref, acc_ref, zout, o_sem,
):
    rows, width = tok_hbm.shape
    topk = ids_hbm.shape[0]
    size = n // groups
    mains = cap // TILE
    rest = cap - mains * TILE
    slot = 1
    while slot < rest:
        slot *= 2
    cuts = TILE // slot
    part = width // cuts
    base = mains * width
    me = lax.axis_index("expert")
    dp = lax.axis_index("dp")
    zone = me // size
    lane = me % size

    plan = PLAN if groups == 4 else PLAN_ONE
    inner = ((zone + 1) // 2) % 2 if groups == 4 else 0
    tail = [step[1] for step in plan if step[0] == "done"]

    def home(k):
        return isinstance(k, int) and k == 0

    def zone_of(k):
        if groups == 4:
            return ((zone // 2 + k // 2) % 2) * 2 + (zone % 2 + k % 2) % 2
        return (zone + k) % groups

    def peer_of(j):
        return (dp + j) % dpn

    def landed(ref, sem):
        pltpu.make_async_copy(ref, ref, sem).wait()

    inputs = [
        pltpu.make_async_copy(src, dst, i_sem.at[i])
        for i, (src, dst) in enumerate(
            ((ids_hbm, ids_ref), (tok_hbm, tok_ref), (router_hbm, router_ref))
        )
    ]
    for load in inputs:
        load.start()

    z_copy = pltpu.make_async_copy(zout, z_ref, o_sem)
    barrier = pltpu.get_barrier_semaphore()

    def greet(j, c):
        pl.semaphore_signal(
            barrier, inc=1, device_id={"expert": (me + j) % n}, device_id_type=MESH
        )
        return c

    lax.fori_loop(1, n, greet, 0)
    for j in range(1, dpn):
        pl.semaphore_signal(
            barrier, inc=1, device_id={"dp": peer_of(j)}, device_id_type=MESH
        )

    inputs[0].wait()
    hot_t = [(ids_ref[k : k + 1, :] == iota((n, rows), 0)) for k in range(topk)]
    all_t = sum(h.astype(F32) for h in hot_t).astype(BF16)
    upper = (iota((rows, rows), 0) < iota((rows, rows), 1)).astype(F32).astype(BF16)
    before_t = dot(all_t, upper)
    pos_t = [
        jnp.sum(jnp.where(h, before_t, 0.0), axis=0, keepdims=True).astype(jnp.int32)
        for h in hot_t
    ]

    def targets(ids, pos):
        out = []
        for m in range(mains):
            inside = (pos >= m * TILE) & (pos < (m + 1) * TILE)
            out.append(jnp.where(inside, ids * TILE + pos - m * TILE, -1))
        for c in range(cuts if rest else 0):
            inside = pos >= mains * TILE
            out.append(jnp.where(inside, ids * TILE + c * slot + pos - mains * TILE, -1))
        return out

    inputs[1].wait()
    for i, src in enumerate((gate_hbm, up_hbm, down_hbm)):
        pltpu.make_async_copy(src.at[0], ffn_ref.at[i], w_sem).start()
    goal_t = [targets(ids_ref[k : k + 1, :], pos_t[k]) for k in range(topk)]
    row_at = iota((size * TILE, rows), 0)

    def dispatch(to, at):
        return pltpu.make_async_remote_copy(
            src_ref=snd.at[to], dst_ref=rx.at[dp, at],
            send_sem=d_send, recv_sem=d_recv.at[at],
            device_id={"expert": to}, device_id_type=MESH,
        )

    def forward(j, at, whose):
        return pltpu.make_async_remote_copy(
            src_ref=rx.at[dp, at], dst_ref=rx.at[whose, at],
            send_sem=f_send, recv_sem=f_recv.at[dpn - 1 - j, at // size],
            device_id={"dp": peer_of(j)}, device_id_type=MESH,
        )

    def send_group(k, entry=False):
        first = zone_of(k) * size
        mine = pl.ds(first, size)

        def pick(i):
            at = row_at + first * TILE
            hit = at == goal_t[0][i]
            for c in range(1, topk):
                hit = hit | (at == goal_t[c][i])
            return hit.astype(F32).astype(BF16)

        for m in range(mains):
            snd[mine, :, m * width : (m + 1) * width] = (
                dot(pick(m), tok_ref[...]).astype(BF16).reshape(size, TILE, width)
            )
        if rest:
            extra = sum(
                dot(pick(mains + c), tok_ref[:, c * part : (c + 1) * part])
                for c in range(cuts)
            )
            snd[mine, :, base:] = extra.astype(BF16).reshape(size, TILE, part)
        if entry:
            pl.semaphore_wait(barrier, n - 1 + dpn - 1)

        def one(j, c):
            to = first + (lane + j) % size
            dispatch(to, me).start()
            return c

        lax.fori_loop(1 if home(k) else 0, size, one, 0)
        if home(k):
            rx[dp, me] = snd[me]
            for q in range(1, dpn):
                forward(q, me, dp).start()

    def order_of(blocks):
        full = blocks * TILE
        at_row, at_col = iota((full, full), 0), iota((full, full), 1)
        per_cut = blocks * slot
        want = ((at_row % per_cut) // slot) * TILE + (at_row // per_cut) * slot + at_row % slot
        return (at_col == want).astype(F32).astype(BF16)

    def part_of(k, half):
        if half is None:
            return zone_of(k) * size, size, 0
        near = lane // (size // 2)
        side = near if half else (near + 1) % 2
        return zone_of(k) * size + side * (size // 2), size // 2, side

    count = size * TILE

    def natural(block):
        blocks = block.shape[0]
        count, per_cut, order = blocks * TILE, blocks * slot, order_of(blocks)
        pieces = [
            block[:, :, m * width : (m + 1) * width].reshape(count, width)
            for m in range(mains)
        ]
        if rest:
            sorted_rows = dot(order, block[:, :, base:].reshape(count, part)).astype(BF16)
            pieces.append(
                jnp.concatenate(
                    [sorted_rows[c * per_cut : (c + 1) * per_cut] for c in range(cuts)],
                    axis=1,
                )
            )
        return pieces

    def blocks_of(rows_out, blocks, store):
        count, order = blocks * TILE, order_of(blocks)
        for m in range(mains):
            store(
                m * width, width,
                rows_out[m * count : (m + 1) * count].reshape(blocks, TILE, width),
            )
        if rest:
            extra = rows_out[mains * count :]
            stacked = jnp.concatenate(
                [extra[:, c * part : (c + 1) * part] for c in range(cuts)], axis=0
            )
            mixed = dot(order, stacked, ((0,), (0,))).astype(BF16)
            store(base, part, mixed.reshape(blocks, TILE, part))

    def expert(block):
        x = jnp.concatenate(natural(block), axis=0)
        gate = dot(x, ffn_ref[0], ((1,), (1,)))
        up = dot(x, ffn_ref[1], ((1,), (1,)))
        hidden = (gate / (1.0 + jnp.exp(-gate)) * up).astype(BF16)
        return dot(hidden, ffn_ref[2])

    def partial_copy(j, t, half):
        first, blocks, _ = part_of(t, half)
        mine = pl.ds(first, blocks)
        return pltpu.make_async_remote_copy(
            src_ref=rx.at[peer_of(j), mine], dst_ref=px.at[dp, mine],
            send_sem=p_send, recv_sem=p_recv.at[dpn - 1 - j, zone_of(t), half or 0],
            device_id={"dp": peer_of(j)}, device_id_type=MESH,
        )

    def give_back(to, at):
        return pltpu.make_async_remote_copy(
            src_ref=fin.at[to], dst_ref=ret.at[at],
            send_sem=r_send, recv_sem=r_recv.at[at // size],
            device_id={"expert": to}, device_id_type=MESH,
        )

    def loss_copy(to, at):
        return pltpu.make_async_remote_copy(
            src_ref=zsnd, dst_ref=zrx.at[at],
            send_sem=z_send, recv_sem=z_recv,
            device_id={"expert": to}, device_id_type=MESH,
        )

    def loss_dp(j, whose):
        return pltpu.make_async_remote_copy(
            src_ref=zmid, dst_ref=zdp.at[whose],
            send_sem=y_send, recv_sem=y_recv,
            device_id={"dp": peer_of(j)}, device_id_type=MESH,
        )

    def route():
        inputs[2].wait()
        logits = dot(tok_ref[...], router_ref[...], ((1,), (1,)))
        top = jnp.max(logits, axis=1, keepdims=True)
        log_total = top + jnp.log(jnp.sum(jnp.exp(logits - top), axis=1, keepdims=True))
        local = jnp.sum(log_total * log_total, axis=0, keepdims=True)
        zsnd[...] = jnp.broadcast_to(local, zsnd.shape)
        zrx[me] = jnp.broadcast_to(local, zsnd.shape)

        def send_loss(j, c):
            loss_copy((me + j) % n, me).start()
            return c

        lax.fori_loop(1, n, send_loss, 0)

        same = (iota((n, n), 0) == iota((n, n), 1)).astype(F32).astype(BF16)
        hot = [dot(h.astype(F32).astype(BF16), same, ((0,), (0,))) > 0.5 for h in hot_t]
        ids = [
            jnp.sum(jnp.where(h, iota((rows, n), 1), 0), axis=1, keepdims=True) for h in hot
        ]
        chosen = [jnp.sum(jnp.where(h, logits, 0.0), axis=1, keepdims=True) for h in hot]
        high = functools.reduce(jnp.maximum, chosen)
        exps = [jnp.exp(c - high) for c in chosen]
        share = [e / sum(exps) for e in exps]
        all_hot = sum(h.astype(F32) for h in hot).astype(BF16)
        lower = (iota((rows, rows), 1) < iota((rows, rows), 0)).astype(F32).astype(BF16)
        before = dot(lower, all_hot)
        pos = [
            jnp.sum(jnp.where(h, before, 0.0), axis=1, keepdims=True).astype(jnp.int32)
            for h in hot
        ]
        goal = [targets(ids[k], pos[k]) for k in range(topk)]

        col_at = iota((rows, n * TILE), 1)
        for i in range(mains + (cuts if rest else 0)):
            w = sum(jnp.where(col_at == goal[k][i], share[k], 0.0) for k in range(topk))
            hi = w.astype(BF16)
            hi_ref[i] = hi
            lo_ref[i] = (w - hi.astype(F32)).astype(BF16)

    def arrive(k, part=None):
        first = zone_of(k) * size

        def one(j, c):
            at = first + (lane + size - j) % size
            dispatch(at, at).wait_recv()
            for q in range(1, dpn):
                forward(q, at, dp).start()
            return c

        if part is None:
            lax.fori_loop(1 if home(k) else 0, size, one, 0)
        else:
            quarter = size // 4
            lax.fori_loop(part * quarter, (part + 1) * quarter, one, 0)

    def own_part(k):
        own[k] = expert(rx[dp, pl.ds(zone_of(k) * size, size)])

    def peer_part(k):
        first = zone_of(k) * size

        def one(q, c):
            whose = peer_of(q)

            landed(rx.at[whose, pl.ds(first, size)], f_recv.at[q - 1, zone_of(k)])
            out = expert(rx[whose, pl.ds(first, size)]).astype(BF16)

            def store(start, wide, value):
                rx[whose, pl.ds(first, size), :, start : start + wide] = value

            blocks_of(out, size, store)
            return c

        lax.fori_loop(1, dpn, one, 0)

    def send_part(k, half=None):
        for q in range(1, dpn):
            partial_copy(q, k, half).start()

    def finish(k, half=None):
        first, blocks, side = part_of(k, half)
        if half is None:
            total = own[k]
        else:
            total = []
            for at, tall in [(m * count, blocks * TILE) for m in range(mains)] + (
                [(mains * count, blocks * slot)] if rest else []
            ):
                total.append(own[k, pl.ds(pl.multiple_of(at + side * tall, 8), tall), :])
            total = jnp.concatenate(total, axis=0)
        for q in range(1, dpn):
            block = px.at[peer_of(q), pl.ds(first, blocks)]
            landed(block, p_recv.at[q - 1, zone_of(k), half or 0])
            total = total + jnp.concatenate(natural(block[...]), axis=0).astype(F32)

        def store(start, wide, value):
            fin[pl.ds(first, blocks), :, start : start + wide] = value

        blocks_of(total.astype(BF16), blocks, store)
        mixed = home(k) and half != 0

        def back(j, c):
            give_back(first + (lane % blocks + j) % blocks, me).start()
            return c

        lax.fori_loop(1 if mixed else 0, blocks, back, 0)
        if mixed:
            ret[me] = fin[me]

    def cut(i, k):
        start = zone_of(k) * size * TILE
        sub = (iota((n * TILE, size * TILE), 0) == iota((n * TILE, size * TILE), 1) + start)
        sub = sub.astype(F32).astype(BF16)
        hi = dot(hi_ref[i], sub).astype(BF16)
        lo = dot(lo_ref[i], sub).astype(BF16)
        return jnp.concatenate([hi, lo], axis=1)

    def weigh(k):
        for i in range(mains + (cuts if rest else 0)):
            for k in range(groups):
                w_ref[i, k] = cut(i, k)

    def take(ks):
        for k in ks:
            here = pl.ds(zone_of(k) * size, size - 1 if home(k) else size)
            landed(ret.at[here], r_recv.at[zone_of(k)])

        def twice(x):
            return jnp.concatenate([x, x], axis=0)

        for c in range(cuts):
            cols = slice(c * part, (c + 1) * part)
            acc = 0.0 if ks == tail[0] else acc_ref[:, cols]
            for k in ks:
                mine = pl.ds(zone_of(k) * size, size)
                for m in range(mains):
                    seen = ret[mine, :, m * width + c * part : m * width + (c + 1) * part]
                    acc = acc + dot(w_ref[m, k], twice(seen.reshape(count, part)))
                if rest:
                    seen = ret[mine, :, base:].reshape(count, part)
                    acc = acc + dot(w_ref[mains + c, k], twice(seen))
            if ks == tail[-1]:
                mix_ref[:, cols] = acc.astype(BF16)
            else:
                acc_ref[:, cols] = acc

    def loads_in(k):
        landed(ffn_ref, w_sem)

    def gather_loss():
        landed(zrx.at[pl.ds(0, n - 1)], z_recv)
        mid = zrx[0]
        for i in range(1, n):
            mid = mid + zrx[i]
        zmid[...] = mid
        zdp[dp] = mid

        for q in range(1, dpn):
            loss_dp(q, dp).start()

    def drain(k):
        landed(snd.at[pl.ds(0, n - 1)], d_send)
        landed(zrx.at[pl.ds(0, n - 1)], z_send)
        landed(rx.at[pl.ds(0, dpn - 1)], f_send)
        landed(px.at[pl.ds(0, dpn - 1)], p_send)
        landed(zdp.at[pl.ds(0, dpn - 1)], y_send)
        landed(zdp.at[pl.ds(0, dpn - 1)], y_recv)
        loss = zdp[dp]
        for q in range(1, dpn):
            loss = loss + zdp[peer_of(q)]
        zout[...] = loss[0:1, 0:1] / F32(rows * n * dpn)
        z_copy.start()

    steps = {
        "send": send_group, "got": arrive, "own": own_part, "peer": peer_part,
        "part": send_part, "end": finish, "done": take, "load": loads_in,
        "route": lambda k: route(), "loss": lambda k: gather_loss(), "weigh": weigh, "drain": drain,
    }
    for op, at, *more in plan:
        with jax.named_scope(f"{op}_{at}_{more}"):
            if op == "done" or not isinstance(at, tuple):
                steps[op](at, *more)
            elif None in at:
                chosen = at[0] if at[1] is None else at[1]
                pl.when(inner == at.index(chosen))(functools.partial(steps[op], chosen, *more))
            else:
                steps[op](at[0] + inner * (at[1] - at[0]), *more)

    z_copy.wait()

    landed(fin.at[pl.ds(0, n - 1)], r_send)


def on_device(n, dpn, tokens, router_weight, route_ids, gate_weight, up_weight, down_weight):
    rows, width = tokens.shape
    topk = route_ids.shape[1]
    experts = router_weight.shape[1]
    assert experts == n and gate_weight.shape[0] == 1
    cap = 5 * rows * topk // (4 * experts)
    groups = 4 if n % 4 == 0 else 1
    mains, rest = cap // TILE, cap % TILE
    slot = 1
    while slot < rest:
        slot *= 2
    block = mains * width + (width * slot // TILE if rest else 0)
    size = n // groups
    in_rows = size * TILE * mains + (size * slot if rest else 0)
    hidden = gate_weight.shape[1]
    vmem = pl.BlockSpec(memory_space=pltpu.VMEM)
    hbm = pl.BlockSpec(memory_space=pl.ANY)
    dma = pltpu.SemaphoreType.DMA
    mixture, loss = pl.pallas_call(
        functools.partial(kernel, n, dpn, cap, groups),
        out_shape=(
            pltpu.VMEM((rows, width), BF16),
            jax.ShapeDtypeStruct((1, 1), F32),
        ),
        in_specs=[hbm] * 6,
        out_specs=(vmem, hbm),
        scratch_shapes=[
            pltpu.VMEM((rows, width), BF16),
            pltpu.VMEM((experts, width), BF16),
            pltpu.VMEM((topk, rows), jnp.int32),
            pltpu.VMEM((n, TILE, block), BF16),
            pltpu.VMEM((dpn, n, TILE, block), BF16),
            pltpu.VMEM((dpn, n, TILE, block), BF16),
            pltpu.VMEM((n, TILE, block), BF16),
            pltpu.VMEM((n, TILE, block), BF16),
            pltpu.VMEM((groups, in_rows, width), F32),
            pltpu.VMEM((3, hidden, width), BF16),
            pltpu.VMEM((8, 128), F32),
            pltpu.VMEM((n, 8, 128), F32),
            pltpu.VMEM((8, 128), F32),
            pltpu.VMEM((dpn, 8, 128), F32),
            dma, dma((n,)), dma, dma((dpn - 1, groups)),
            dma, dma((dpn - 1, groups, 2)), dma, dma((groups,)),
            dma, dma, dma, dma, dma, dma((3,)),
            pltpu.VMEM((mains + (TILE // slot if rest else 0), rows, n * TILE), BF16),
            pltpu.VMEM((mains + (TILE // slot if rest else 0), rows, n * TILE), BF16),
            pltpu.VMEM((mains + (TILE // slot if rest else 0), groups, rows, 2 * size * TILE), BF16),
            pltpu.VMEM((rows, width), F32),
            pltpu.VMEM((1, 1), F32),
            dma,
        ],
        compiler_params=pltpu.CompilerParams(
            collective_id=0, has_side_effects=True, vmem_limit_bytes=60 * 1024 * 1024
        ),
    )(tokens, router_weight.T, route_ids.T, gate_weight, up_weight, down_weight)
    return mixture, loss[0, 0]


def solution(mesh):
    in_specs = (
        P(("dp", "expert"), None),
        P(),
        P(("dp", "expert"), None),
        P("expert", "dp", None),
        P("expert", "dp", None),
        P("expert", "dp", None),
    )
    out_specs = (P(("dp", "expert"), None), P())
    return jax.shard_map(
        functools.partial(on_device, mesh.shape["expert"], mesh.shape["dp"]),
        mesh=mesh, in_specs=in_specs, out_specs=out_specs, check_vma=False,
    )
```

```python
import functools

import jax
import jax.numpy as jnp
from jax import lax
from jax.experimental import pallas as pl
from jax.experimental.pallas import tpu as pltpu
from jax.sharding import PartitionSpec as P

MESH = pl.DeviceIdType.MESH
F32 = jnp.float32
BF16 = jnp.bfloat16
TILE = 16
NO = None
PLAN = (
    ("share", 0, True), ("send", (2, 1)), ("share", 1), ("send", 0), ("send", (1, 2)), ("send", 3),
    ("share", (2, NO)), ("share", (3, NO)),
    ("load", 0), ("pass", (NO, 2), 0), ("pass", (NO, 2), 1), ("pass", (NO, 2), 2), ("pass", (NO, 2), 3),
    ("share", (NO, 2)), ("share", (NO, 3)), ("got", 0), ("own", 0), ("route", 0),
    ("got", (1, NO)), ("own", (1, 2)), ("weigh", 0),
    ("pass", (2, NO), 0), ("pass", (2, NO), 1),
    ("peer", (NO, 2)), ("part", (NO, 2), 0), ("part", (NO, 2), 1), ("relay", 0),
    ("pass", (2, NO), 2), ("pass", (2, NO), 3), ("got", (NO, 1)), ("own", (2, 1)),
    ("pass", 3, 0), ("pass", 3, 1), ("end", (NO, 2), 0), ("pass", 3, 2), ("end", (NO, 2), 1), ("pass", 3, 3),
    ("own", (NO, 3)), ("peer", (2, 1)), ("part", (2, 1), 0), ("part", (2, 1), 1), ("own", (3, NO)),
    ("peer", 3), ("part", 3, 0), ("part", 3, 1), ("end", (2, NO), 0),
    ("peer", (1, 0)), ("part", (1, 0), 0),
    ("peer", (0, NO)), ("part", (0, NO), 0), ("part", (1, NO), 1), ("part", 0, 1),
    ("end", (2, 1), (1, 0)), ("end", (3, 1), (0, 1)), ("loss", 0), ("end", 3, (1, 0)),
    ("end", (1, 3), (0, 1)), ("end", 0, 0), ("end", (1, NO), 1), ("done", 2, "first"), ("end", 0, 1),
    ("drain", 0), ("done", (3, 1)), ("done", 0), ("done", (1, 3), "last"),
)
ORDER_ONE = ("send", "load", "relay", "got", "route", "weigh", "own", "peer", "part", "end", "loss", "drain", "done")
PLAN_ONE = (("share", 0, True), ("share", 1), ("share", 2), ("share", 3)) + tuple(
    (op, 0, "only") if op == "done" else (op, 0) for op in ORDER_ONE
)


def dot(a, b, dims=((1,), (0,))):
    return lax.dot_general(a, b, (dims, ((), ())), preferred_element_type=F32)


def iota(shape, axis):
    return lax.broadcasted_iota(jnp.int32, shape, axis)


def kernel(
    n, dpn, cap, groups,
    tok_hbm, router_hbm, ids_hbm, gate_hbm, up_hbm, down_hbm,
    mix_ref, z_ref,
    tok_ref, router_ref, ids_ref, snd, rx, px, fin, ret, own, ffn_ref, zsnd, zrx, zmid, zdp,
    d_send, d_recv, f_send, f_recv, p_send, p_recv, r_send, r_recv,
    z_send, z_recv, y_send, y_recv, w_sem, i_sem,
    hi_ref, lo_ref, w_ref, acc_ref, zout, o_sem,
    peer_tok, peer_ids, out_ref, s_send, s_recv, t_send, t_recv, e_send,
):
    rows, width = tok_hbm.shape
    topk = ids_hbm.shape[0]
    size = n // groups
    mains = cap // TILE
    rest = cap - mains * TILE
    slot = 1
    while slot < rest:
        slot *= 2
    cuts = TILE // slot
    part = width // cuts
    base = mains * width
    me = lax.axis_index("expert")
    dp = lax.axis_index("dp")
    zone = me // size
    lane = me % size

    plan = PLAN if groups == 4 else PLAN_ONE
    inner = ((zone + 1) // 2) % 2 if groups == 4 else 0

    near = 2 if groups == 4 else 1

    def home(k):
        return isinstance(k, int) and k == 0

    def zone_of(k):
        if groups == 4:
            return ((zone // 2 + k // 2) % 2) * 2 + (zone % 2 + k % 2) % 2
        return (zone + k) % groups

    def peer_of(j):
        return (dp + j) % dpn

    def landed(ref, sem):
        pltpu.make_async_copy(ref, ref, sem).wait()

    inputs = [
        pltpu.make_async_copy(src, dst, i_sem.at[i])
        for i, (src, dst) in enumerate(
            ((ids_hbm, ids_ref), (tok_hbm, tok_ref), (router_hbm, router_ref))
        )
    ]
    for load in inputs:
        load.start()

    z_copy = pltpu.make_async_copy(zout, z_ref, o_sem)
    barrier = pltpu.get_barrier_semaphore()

    def greet(j, c):
        pl.semaphore_signal(
            barrier, inc=1, device_id={"expert": (me + j) % n}, device_id_type=MESH
        )
        return c

    lax.fori_loop(1, n, greet, 0)
    for j in range(1, dpn):
        pl.semaphore_signal(
            barrier, inc=1, device_id={"dp": peer_of(j)}, device_id_type=MESH
        )

    inputs[0].wait()
    upper = (iota((rows, rows), 0) < iota((rows, rows), 1)).astype(F32).astype(BF16)

    def hot_of(ids):
        return [(ids[k : k + 1, :] == iota((n, rows), 0)) for k in range(topk)]

    def goals(ids):
        hot = hot_of(ids)
        before = dot(sum(h.astype(F32) for h in hot).astype(BF16), upper)
        pos = [
            jnp.sum(jnp.where(h, before, 0.0), axis=0, keepdims=True).astype(jnp.int32)
            for h in hot
        ]
        return [targets(ids[k : k + 1, :], pos[k]) for k in range(topk)]

    def targets(ids, pos):
        out = []
        for m in range(mains):
            inside = (pos >= m * TILE) & (pos < (m + 1) * TILE)
            out.append(jnp.where(inside, ids * TILE + pos - m * TILE, -1))
        for c in range(cuts if rest else 0):
            inside = pos >= mains * TILE
            out.append(jnp.where(inside, ids * TILE + c * slot + pos - mains * TILE, -1))
        return out

    hot_t = hot_of(ids_ref[...])
    goal_t = goals(ids_ref[...])
    inputs[1].wait()
    for i, src in enumerate((gate_hbm, up_hbm, down_hbm)):
        pltpu.make_async_copy(src.at[0], ffn_ref.at[i], w_sem).start()
    row_at = iota((size * TILE, rows), 0)

    def dispatch(to, at):
        return pltpu.make_async_remote_copy(
            src_ref=snd.at[to], dst_ref=rx.at[dp, at],
            send_sem=d_send, recv_sem=d_recv.at[at],
            device_id={"expert": to}, device_id_type=MESH,
        )

    def forward(j, at, whose):
        return pltpu.make_async_remote_copy(
            src_ref=rx.at[dp, at], dst_ref=rx.at[whose, at],
            send_sem=f_send, recv_sem=f_recv.at[dpn - 1 - j, at // size],
            device_id={"dp": peer_of(j)}, device_id_type=MESH,
        )

    def gather(tokens, goal, first, store):
        def pick(i):
            at = row_at + first * TILE
            hit = at == goal[0][i]
            for c in range(1, topk):
                hit = hit | (at == goal[c][i])
            return hit.astype(F32).astype(BF16)

        for m in range(mains):
            chosen = dot(pick(m), tokens[...]).astype(BF16)
            store(m * width, width, chosen.reshape(size, TILE, width))
        if rest:
            extra = sum(
                dot(pick(mains + c), tokens[:, c * part : (c + 1) * part])
                for c in range(cuts)
            )
            store(base, part, extra.astype(BF16).reshape(size, TILE, part))

    def send_group(k):
        first = zone_of(k) * size

        def store(start, wide, value):
            snd[pl.ds(first, size), :, start : start + wide] = value

        gather(tok_ref, goal_t, first, store)

        def one(j, c):
            to = first + (lane + j) % size
            dispatch(to, me).start()
            return c

        lax.fori_loop(1 if home(k) else 0, size, one, 0)
        if home(k):
            rx[dp, me] = snd[me]

    def share(c, entry=False):
        if entry:
            pl.semaphore_wait(barrier, n - 1 + dpn - 1)
        mine = pl.ds(c * (rows // 4), rows // 4)
        for q in range(1, dpn):
            pltpu.make_async_remote_copy(
                src_ref=tok_ref.at[mine], dst_ref=peer_tok.at[dpn - 1 - q, mine],
                send_sem=s_send, recv_sem=s_recv.at[dpn - 1 - q],
                device_id={"dp": peer_of(q)}, device_id_type=MESH,
            ).start()
            if entry:
                pltpu.make_async_remote_copy(
                    src_ref=ids_ref, dst_ref=peer_ids.at[dpn - 1 - q],
                    send_sem=t_send, recv_sem=t_recv.at[dpn - 1 - q],
                    device_id={"dp": peer_of(q)}, device_id_type=MESH,
                ).start()

    def relay(unused):
        def one_peer(q, c):
            whose = peer_of(q)
            landed(peer_ids.at[q - 1], t_recv.at[q - 1])
            goal = goals(peer_ids[q - 1])
            landed(peer_tok.at[q - 1], s_recv.at[q - 1])
            for k in range(near):
                first = zone_of(k) * size

                def store(start, wide, value, k=k):
                    out_ref[q - 1, k * size : (k + 1) * size, :, start : start + wide] = value

                gather(peer_tok.at[q - 1], goal, first, store)

                def one(j, c2, k=k, first=first):
                    to = (lane + j) % size
                    pltpu.make_async_remote_copy(
                        src_ref=out_ref.at[q - 1, k * size + to], dst_ref=rx.at[whose, me],
                        send_sem=e_send, recv_sem=f_recv.at[q - 1, zone],
                        device_id={"expert": first + to}, device_id_type=MESH,
                    ).start()
                    return c2

                lax.fori_loop(1 if k == 0 else 0, size, one, 0)
            rx[whose, me] = out_ref[q - 1, lane]
            return c

        lax.fori_loop(1, dpn, one_peer, 0)

    def order_of(blocks):
        full = blocks * TILE
        at_row, at_col = iota((full, full), 0), iota((full, full), 1)
        per_cut = blocks * slot
        want = ((at_row % per_cut) // slot) * TILE + (at_row // per_cut) * slot + at_row % slot
        return (at_col == want).astype(F32).astype(BF16)

    def part_of(k, half):
        if half is None:
            return zone_of(k) * size, size, 0
        near = lane // (size // 2)
        side = near if half else (near + 1) % 2
        return zone_of(k) * size + side * (size // 2), size // 2, side

    count = size * TILE

    def natural(block):
        blocks = block.shape[0]
        count, per_cut, order = blocks * TILE, blocks * slot, order_of(blocks)
        pieces = [
            block[:, :, m * width : (m + 1) * width].reshape(count, width)
            for m in range(mains)
        ]
        if rest:
            sorted_rows = dot(order, block[:, :, base:].reshape(count, part)).astype(BF16)
            pieces.append(
                jnp.concatenate(
                    [sorted_rows[c * per_cut : (c + 1) * per_cut] for c in range(cuts)],
                    axis=1,
                )
            )
        return pieces

    def blocks_of(rows_out, blocks, store):
        count, order = blocks * TILE, order_of(blocks)
        for m in range(mains):
            store(
                m * width, width,
                rows_out[m * count : (m + 1) * count].reshape(blocks, TILE, width),
            )
        if rest:
            extra = rows_out[mains * count :]
            stacked = jnp.concatenate(
                [extra[:, c * part : (c + 1) * part] for c in range(cuts)], axis=0
            )
            mixed = dot(order, stacked, ((0,), (0,))).astype(BF16)
            store(base, part, mixed.reshape(blocks, TILE, part))

    def expert(block):
        x = jnp.concatenate(natural(block), axis=0)
        gate = dot(x, ffn_ref[0], ((1,), (1,)))
        up = dot(x, ffn_ref[1], ((1,), (1,)))
        hidden = (gate / (1.0 + jnp.exp(-gate)) * up).astype(BF16)
        return dot(hidden, ffn_ref[2])

    def partial_copy(j, t, half):
        first, blocks, _ = part_of(t, half)
        mine = pl.ds(first, blocks)
        return pltpu.make_async_remote_copy(
            src_ref=rx.at[peer_of(j), mine], dst_ref=px.at[dp, mine],
            send_sem=p_send, recv_sem=p_recv.at[dpn - 1 - j, zone_of(t), half or 0],
            device_id={"dp": peer_of(j)}, device_id_type=MESH,
        )

    def give_back(to, at):
        return pltpu.make_async_remote_copy(
            src_ref=fin.at[to], dst_ref=ret.at[at],
            send_sem=r_send, recv_sem=r_recv.at[at // size],
            device_id={"expert": to}, device_id_type=MESH,
        )

    def loss_copy(to, at):
        return pltpu.make_async_remote_copy(
            src_ref=zsnd, dst_ref=zrx.at[at],
            send_sem=z_send, recv_sem=z_recv,
            device_id={"expert": to}, device_id_type=MESH,
        )

    def loss_dp(j, whose):
        return pltpu.make_async_remote_copy(
            src_ref=zmid, dst_ref=zdp.at[whose],
            send_sem=y_send, recv_sem=y_recv,
            device_id={"dp": peer_of(j)}, device_id_type=MESH,
        )

    def route():
        inputs[2].wait()
        logits = dot(tok_ref[...], router_ref[...], ((1,), (1,)))
        top = jnp.max(logits, axis=1, keepdims=True)
        log_total = top + jnp.log(jnp.sum(jnp.exp(logits - top), axis=1, keepdims=True))
        local = jnp.sum(log_total * log_total, axis=0, keepdims=True)
        zsnd[...] = jnp.broadcast_to(local, zsnd.shape)
        zrx[me] = jnp.broadcast_to(local, zsnd.shape)

        def send_loss(j, c):
            loss_copy((me + j) % n, me).start()
            return c

        lax.fori_loop(1, n, send_loss, 0)

        same = (iota((n, n), 0) == iota((n, n), 1)).astype(F32).astype(BF16)
        hot = [dot(h.astype(F32).astype(BF16), same, ((0,), (0,))) > 0.5 for h in hot_t]
        ids = [
            jnp.sum(jnp.where(h, iota((rows, n), 1), 0), axis=1, keepdims=True) for h in hot
        ]
        chosen = [jnp.sum(jnp.where(h, logits, 0.0), axis=1, keepdims=True) for h in hot]
        high = functools.reduce(jnp.maximum, chosen)
        exps = [jnp.exp(c - high) for c in chosen]
        share = [e / sum(exps) for e in exps]
        all_hot = sum(h.astype(F32) for h in hot).astype(BF16)
        lower = (iota((rows, rows), 1) < iota((rows, rows), 0)).astype(F32).astype(BF16)
        before = dot(lower, all_hot)
        pos = [
            jnp.sum(jnp.where(h, before, 0.0), axis=1, keepdims=True).astype(jnp.int32)
            for h in hot
        ]
        goal = [targets(ids[k], pos[k]) for k in range(topk)]

        col_at = iota((rows, n * TILE), 1)
        for i in range(mains + (cuts if rest else 0)):
            w = sum(jnp.where(col_at == goal[k][i], share[k], 0.0) for k in range(topk))
            hi = w.astype(BF16)
            hi_ref[i] = hi
            lo_ref[i] = (w - hi.astype(F32)).astype(BF16)

    def arrive(k, part=None, onward=False):
        first = zone_of(k) * size

        def one(j, c):
            at = first + (lane + size - j) % size
            dispatch(at, at).wait_recv()
            for q in range(1, dpn if onward else 1):
                forward(q, at, dp).start()
            return c

        if part is None:
            lax.fori_loop(1 if home(k) else 0, size, one, 0)
        else:
            quarter = size // 4
            lax.fori_loop(part * quarter, (part + 1) * quarter, one, 0)

    def own_part(k):
        own[k] = expert(rx[dp, pl.ds(zone_of(k) * size, size)])

    def peer_part(k):
        first = zone_of(k) * size

        def one(q, c):
            whose = peer_of(q)

            come = pl.ds(first, size - 1 if home(k) else size)
            landed(rx.at[whose, come], f_recv.at[q - 1, zone_of(k)])
            out = expert(rx[whose, pl.ds(first, size)]).astype(BF16)

            def store(start, wide, value):
                rx[whose, pl.ds(first, size), :, start : start + wide] = value

            blocks_of(out, size, store)
            return c

        lax.fori_loop(1, dpn, one, 0)

    def send_part(k, half=None):
        for q in range(1, dpn):
            partial_copy(q, k, half).start()

    def finish(k, half=None):
        first, blocks, side = part_of(k, half)
        if half is None:
            total = own[k]
        else:
            total = []
            for at, tall in [(m * count, blocks * TILE) for m in range(mains)] + (
                [(mains * count, blocks * slot)] if rest else []
            ):
                total.append(own[k, pl.ds(pl.multiple_of(at + side * tall, 8), tall), :])
            total = jnp.concatenate(total, axis=0)
        for q in range(1, dpn):
            block = px.at[peer_of(q), pl.ds(first, blocks)]
            landed(block, p_recv.at[q - 1, zone_of(k), half or 0])
            total = total + jnp.concatenate(natural(block[...]), axis=0).astype(F32)

        def store(start, wide, value):
            fin[pl.ds(first, blocks), :, start : start + wide] = value

        blocks_of(total.astype(BF16), blocks, store)
        mixed = home(k) and half != 0

        def back(j, c):
            give_back(first + (lane % blocks + j) % blocks, me).start()
            return c

        lax.fori_loop(1 if mixed else 0, blocks, back, 0)
        if mixed:
            ret[me] = fin[me]

    def cut(i, k):
        start = zone_of(k) * size * TILE
        sub = (iota((n * TILE, size * TILE), 0) == iota((n * TILE, size * TILE), 1) + start)
        sub = sub.astype(F32).astype(BF16)
        hi = dot(hi_ref[i], sub).astype(BF16)
        lo = dot(lo_ref[i], sub).astype(BF16)
        return jnp.concatenate([hi, lo], axis=1)

    def weigh(k):
        for i in range(mains + (cuts if rest else 0)):
            for k in range(groups):
                w_ref[i, k] = cut(i, k)

    def take(k, place=""):
        here = pl.ds(zone_of(k) * size, size - 1 if home(k) else size)
        landed(ret.at[here], r_recv.at[zone_of(k)])

        def twice(x):
            return jnp.concatenate([x, x], axis=0)

        mine = pl.ds(zone_of(k) * size, size)
        for c in range(cuts):
            cols = slice(c * part, (c + 1) * part)
            acc = 0.0 if place in ("first", "only") else acc_ref[:, cols]
            for m in range(mains):
                seen = ret[mine, :, m * width + c * part : m * width + (c + 1) * part]
                acc = acc + dot(w_ref[m, k], twice(seen.reshape(count, part)))
            if rest:
                seen = ret[mine, :, base:].reshape(count, part)
                acc = acc + dot(w_ref[mains + c, k], twice(seen))
            if place in ("last", "only"):
                mix_ref[:, cols] = acc.astype(BF16)
            else:
                acc_ref[:, cols] = acc

    def loads_in(k):
        landed(ffn_ref, w_sem)

    def gather_loss():
        landed(zrx.at[pl.ds(0, n - 1)], z_recv)
        mid = zrx[0]
        for i in range(1, n):
            mid = mid + zrx[i]
        zmid[...] = mid
        zdp[dp] = mid

        for q in range(1, dpn):
            loss_dp(q, dp).start()

    def drain(k):
        landed(snd.at[pl.ds(0, n - 1)], d_send)
        landed(zrx.at[pl.ds(0, n - 1)], z_send)
        if groups > near:
            landed(rx.at[pl.ds(0, dpn - 1), pl.ds(0, (groups - near) * size)], f_send)
        landed(peer_tok, s_send)
        landed(peer_ids, t_send)
        landed(out_ref.at[pl.ds(0, dpn - 1), pl.ds(0, near * size - 1)], e_send)
        landed(px.at[pl.ds(0, dpn - 1)], p_send)
        landed(zdp.at[pl.ds(0, dpn - 1)], y_send)
        landed(zdp.at[pl.ds(0, dpn - 1)], y_recv)
        loss = zdp[dp]
        for q in range(1, dpn):
            loss = loss + zdp[peer_of(q)]
        zout[...] = loss[0:1, 0:1] / F32(rows * n * dpn)
        z_copy.start()

    steps = {
        "send": send_group, "got": arrive, "share": share, "relay": relay,
        "pass": functools.partial(arrive, onward=True),
        "own": own_part, "peer": peer_part,
        "part": send_part, "end": finish, "done": take, "load": loads_in,
        "route": lambda k: route(), "loss": lambda k: gather_loss(), "weigh": weigh, "drain": drain,
    }
    for op, at, *more in plan:
        with jax.named_scope(f"{op}_{at}_{more}"):
            split = any(isinstance(m, tuple) for m in more)
            if not (split or isinstance(at, tuple)):
                steps[op](at, *more)
            elif split or None in at or 0 in at:
                for kind in range(2):
                    first, *rest_of = [m[kind] if isinstance(m, tuple) else m for m in (at, *more)]
                    if first is not None:
                        pl.when(inner == kind)(functools.partial(steps[op], first, *rest_of))
            else:
                steps[op](at[0] + inner * (at[1] - at[0]), *more)

    z_copy.wait()

    landed(fin.at[pl.ds(0, n - 1)], r_send)


def on_device(n, dpn, tokens, router_weight, route_ids, gate_weight, up_weight, down_weight):
    rows, width = tokens.shape
    topk = route_ids.shape[1]
    experts = router_weight.shape[1]
    assert experts == n and gate_weight.shape[0] == 1
    cap = 5 * rows * topk // (4 * experts)
    groups = 4 if n % 4 == 0 else 1
    mains, rest = cap // TILE, cap % TILE
    slot = 1
    while slot < rest:
        slot *= 2
    block = mains * width + (width * slot // TILE if rest else 0)
    size = n // groups
    in_rows = size * TILE * mains + (size * slot if rest else 0)
    hidden = gate_weight.shape[1]
    vmem = pl.BlockSpec(memory_space=pltpu.VMEM)
    hbm = pl.BlockSpec(memory_space=pl.ANY)
    dma = pltpu.SemaphoreType.DMA
    mixture, loss = pl.pallas_call(
        functools.partial(kernel, n, dpn, cap, groups),
        out_shape=(
            pltpu.VMEM((rows, width), BF16),
            jax.ShapeDtypeStruct((1, 1), F32),
        ),
        in_specs=[hbm] * 6,
        out_specs=(vmem, hbm),
        scratch_shapes=[
            pltpu.VMEM((rows, width), BF16),
            pltpu.VMEM((experts, width), BF16),
            pltpu.VMEM((topk, rows), jnp.int32),
            pltpu.VMEM((n, TILE, block), BF16),
            pltpu.VMEM((dpn, n, TILE, block), BF16),
            pltpu.VMEM((dpn, n, TILE, block), BF16),
            pltpu.VMEM((n, TILE, block), BF16),
            pltpu.VMEM((n, TILE, block), BF16),
            pltpu.VMEM((groups, in_rows, width), F32),
            pltpu.VMEM((3, hidden, width), BF16),
            pltpu.VMEM((8, 128), F32),
            pltpu.VMEM((n, 8, 128), F32),
            pltpu.VMEM((8, 128), F32),
            pltpu.VMEM((dpn, 8, 128), F32),
            dma, dma((n,)), dma, dma((dpn - 1, groups)),
            dma, dma((dpn - 1, groups, 2)), dma, dma((groups,)),
            dma, dma, dma, dma, dma, dma((3,)),
            pltpu.VMEM((mains + (TILE // slot if rest else 0), rows, n * TILE), BF16),
            pltpu.VMEM((mains + (TILE // slot if rest else 0), rows, n * TILE), BF16),
            pltpu.VMEM((mains + (TILE // slot if rest else 0), groups, rows, 2 * size * TILE), BF16),
            pltpu.VMEM((rows, width), F32),
            pltpu.VMEM((1, 1), F32),
            dma,
            pltpu.VMEM((dpn - 1, rows, width), BF16),
            pltpu.VMEM((dpn - 1, topk, rows), jnp.int32),
            pltpu.VMEM((dpn - 1, (2 if groups == 4 else 1) * size, TILE, block), BF16),
            dma, dma((dpn - 1,)), dma, dma((dpn - 1,)), dma,
        ],
        compiler_params=pltpu.CompilerParams(
            collective_id=0, has_side_effects=True, vmem_limit_bytes=60 * 1024 * 1024
        ),
    )(tokens, router_weight.T, route_ids.T, gate_weight, up_weight, down_weight)
    return mixture, loss[0, 0]


def solution(mesh):
    in_specs = (
        P(("dp", "expert"), None),
        P(),
        P(("dp", "expert"), None),
        P("expert", "dp", None),
        P("expert", "dp", None),
        P("expert", "dp", None),
    )
    out_specs = (P(("dp", "expert"), None), P())
    return jax.shard_map(
        functools.partial(on_device, mesh.shape["expert"], mesh.shape["dp"]),
        mesh=mesh, in_specs=in_specs, out_specs=out_specs, check_vma=False,
    )
```

```python
import functools

import jax
import jax.numpy as jnp
from jax import lax
from jax.experimental import pallas as pl
from jax.experimental.pallas import tpu as pltpu
from jax.sharding import PartitionSpec as P

MESH = pl.DeviceIdType.MESH
F32 = jnp.float32
BF16 = jnp.bfloat16
TILE = 16
NO = None
PLAN = (
    ('share', 0, True),
    ('send', (2, 1)),
    ('share', 1),
    ('send', 0),
    ('send', (1, 2)),
    ('pass', (None, 2), 1),
    ('send', 3),
    ('load', (None, 0)),
    ('pass', (None, 2), 0),
    ('pass', (None, 2), 2),
    ('pass', (None, 2), 3),
    ('share', 2),
    ('share', 3),
    ('load', (0, None)),
    ('got', 0),
    ('own', 0),
    ('route', 0),
    ('got', (1, None)),
    ('pass', (2, None), 1),
    ('own', (1, 2)),
    ('weigh', 0),
    ('pass', (2, None), 0),
    ('peer', (None, 2)),
    ('part', (None, 2), 0),
    ('part', (None, 2), 1),
    ('relay', 0),
    ('pass', (2, None), 2),
    ('pass', (2, None), 3),
    ('got', (None, 1)),
    ('own', (2, 1)),
    ('pass', 3, 0),
    ('pass', 3, 1),
    ('end', (None, 2), 0),
    ('pass', 3, 2),
    ('end', (None, 2), 1),
    ('pass', 3, 3),
    ('peer', (2, None)),
    ('part', (2, None), 0),
    ('part', (2, None), 1),
    ('own', 3),
    ('peer', (3, 1)),
    ('part', (3, 1), 0),
    ('part', (3, 1), 1),
    ('end', (2, None), 0),
    ('peer', (1, 3)),
    ('part', (1, 3), 0),
    ('part', (None, 3), 1),
    ('peer', 0),
    ('part', 0, 0),
    ('part', (1, None), 1),
    ('part', 0, 1),
    ('end', (2, None), 1),
    ('end', (3, 1), 0),
    ('loss', (0, None)),
    ('end', (3, 1), 1),
    ('loss', (None, 0)),
    ('end', (1, 3), 0),
    ('end', (0, None), 0),
    ('end', (1, 3), 1),
    ('end', (None, 0), 0),
    ('done', 2, 'first'),
    ('end', 0, 1),
    ('drain', 0),
    ('done', (3, 1)),
    ('done', 0),
    ('done', (1, 3), 'last'),
)
ORDER_ONE = ("send", "load", "relay", "got", "route", "weigh", "own", "peer", "part", "end", "loss", "drain", "done")
PLAN_ONE = (("share", 0, True), ("share", 1), ("share", 2), ("share", 3)) + tuple(
    (op, 0, "only") if op == "done" else (op, 0) for op in ORDER_ONE
)


def dot(a, b, dims=((1,), (0,))):
    return lax.dot_general(a, b, (dims, ((), ())), preferred_element_type=F32)


def iota(shape, axis):
    return lax.broadcasted_iota(jnp.int32, shape, axis)


def kernel(
    n, dpn, cap, groups,
    tok_hbm, router_hbm, ids_hbm, gate_hbm, up_hbm, down_hbm,
    mix_ref, z_ref,
    tok_ref, router_ref, ids_ref, snd, rx, px, fin, ret, own, ffn_ref, zsnd, zrx, zmid, zdp,
    d_send, d_recv, f_send, f_recv, p_send, p_recv, r_send, r_recv,
    z_send, z_recv, y_send, y_recv, w_sem, i_sem,
    hi_ref, lo_ref, w_ref, acc_ref, zout, o_sem,
    peer_tok, peer_ids, out_ref, s_send, s_recv, t_send, t_recv, e_send,
):
    rows, width = tok_hbm.shape
    topk = ids_hbm.shape[0]
    size = n // groups
    mains = cap // TILE
    rest = cap - mains * TILE
    slot = 1
    while slot < rest:
        slot *= 2
    cuts = TILE // slot
    part = width // cuts
    base = mains * width
    me = lax.axis_index("expert")
    dp = lax.axis_index("dp")
    zone = me // size
    lane = me % size

    plan = PLAN if groups == 4 else PLAN_ONE
    inner = ((zone + 1) // 2) % 2 if groups == 4 else 0

    near = 2 if groups == 4 else 1

    def home(k):
        return isinstance(k, int) and k == 0

    def zone_of(k):
        if groups == 4:
            return ((zone // 2 + k // 2) % 2) * 2 + (zone % 2 + k % 2) % 2
        return (zone + k) % groups

    def peer_of(j):
        return (dp + j) % dpn

    def landed(ref, sem):
        pltpu.make_async_copy(ref, ref, sem).wait()

    inputs = [
        pltpu.make_async_copy(src, dst, i_sem.at[i])
        for i, (src, dst) in enumerate(
            ((ids_hbm, ids_ref), (tok_hbm, tok_ref), (router_hbm, router_ref))
        )
    ]
    for load in inputs:
        load.start()

    z_copy = pltpu.make_async_copy(zout, z_ref, o_sem)
    barrier = pltpu.get_barrier_semaphore()

    def greet(j, c):
        pl.semaphore_signal(
            barrier, inc=1, device_id={"expert": (me + j) % n}, device_id_type=MESH
        )
        return c

    lax.fori_loop(1, n, greet, 0)
    for j in range(1, dpn):
        pl.semaphore_signal(
            barrier, inc=1, device_id={"dp": peer_of(j)}, device_id_type=MESH
        )

    inputs[0].wait()
    upper = (iota((rows, rows), 0) < iota((rows, rows), 1)).astype(F32).astype(BF16)

    def hot_of(ids):
        return [(ids[k : k + 1, :] == iota((n, rows), 0)) for k in range(topk)]

    def goals(ids):
        hot = hot_of(ids)
        before = dot(sum(h.astype(F32) for h in hot).astype(BF16), upper)
        pos = [
            jnp.sum(jnp.where(h, before, 0.0), axis=0, keepdims=True).astype(jnp.int32)
            for h in hot
        ]
        return [targets(ids[k : k + 1, :], pos[k]) for k in range(topk)]

    def targets(ids, pos):
        out = []
        for m in range(mains):
            inside = (pos >= m * TILE) & (pos < (m + 1) * TILE)
            out.append(jnp.where(inside, ids * TILE + pos - m * TILE, -1))
        for c in range(cuts if rest else 0):
            inside = pos >= mains * TILE
            out.append(jnp.where(inside, ids * TILE + c * slot + pos - mains * TILE, -1))
        return out

    hot_t = hot_of(ids_ref[...])
    goal_t = goals(ids_ref[...])
    inputs[1].wait()
    for i, src in enumerate((gate_hbm, up_hbm, down_hbm)):
        pltpu.make_async_copy(src.at[0], ffn_ref.at[i], w_sem).start()
    row_at = iota((size * TILE, rows), 0)

    def dispatch(to, at):
        return pltpu.make_async_remote_copy(
            src_ref=snd.at[to], dst_ref=rx.at[dp, at],
            send_sem=d_send, recv_sem=d_recv.at[at],
            device_id={"expert": to}, device_id_type=MESH,
        )

    def forward(j, at, whose):
        return pltpu.make_async_remote_copy(
            src_ref=rx.at[dp, at], dst_ref=rx.at[whose, at],
            send_sem=f_send, recv_sem=f_recv.at[dpn - 1 - j, at // size],
            device_id={"dp": peer_of(j)}, device_id_type=MESH,
        )

    def gather(tokens, goal, first, store):
        def pick(i):
            at = row_at + first * TILE
            hit = at == goal[0][i]
            for c in range(1, topk):
                hit = hit | (at == goal[c][i])
            return hit.astype(F32).astype(BF16)

        for m in range(mains):
            chosen = dot(pick(m), tokens[...]).astype(BF16)
            store(m * width, width, chosen.reshape(size, TILE, width))
        if rest:
            extra = sum(
                dot(pick(mains + c), tokens[:, c * part : (c + 1) * part])
                for c in range(cuts)
            )
            store(base, part, extra.astype(BF16).reshape(size, TILE, part))

    def send_group(k):
        first = zone_of(k) * size

        def store(start, wide, value):
            snd[pl.ds(first, size), :, start : start + wide] = value

        gather(tok_ref, goal_t, first, store)

        def one(j, c):
            to = first + (lane + j) % size
            dispatch(to, me).start()
            return c

        lax.fori_loop(1 if home(k) else 0, size, one, 0)
        if home(k):
            rx[dp, me] = snd[me]

    def share(c, entry=False):
        if entry:
            pl.semaphore_wait(barrier, n - 1 + dpn - 1)
        mine = pl.ds(c * (rows // 4), rows // 4)
        for q in range(1, dpn):
            pltpu.make_async_remote_copy(
                src_ref=tok_ref.at[mine], dst_ref=peer_tok.at[dpn - 1 - q, mine],
                send_sem=s_send, recv_sem=s_recv.at[dpn - 1 - q],
                device_id={"dp": peer_of(q)}, device_id_type=MESH,
            ).start()
            if entry:
                pltpu.make_async_remote_copy(
                    src_ref=ids_ref, dst_ref=peer_ids.at[dpn - 1 - q],
                    send_sem=t_send, recv_sem=t_recv.at[dpn - 1 - q],
                    device_id={"dp": peer_of(q)}, device_id_type=MESH,
                ).start()

    def relay(unused):
        def one_peer(q, c):
            whose = peer_of(q)
            landed(peer_ids.at[q - 1], t_recv.at[q - 1])
            goal = goals(peer_ids[q - 1])
            landed(peer_tok.at[q - 1], s_recv.at[q - 1])
            for k in range(near):
                first = zone_of(k) * size

                def store(start, wide, value, k=k):
                    out_ref[q - 1, k * size : (k + 1) * size, :, start : start + wide] = value

                gather(peer_tok.at[q - 1], goal, first, store)

                def one(j, c2, k=k, first=first):
                    to = (lane + j) % size
                    pltpu.make_async_remote_copy(
                        src_ref=out_ref.at[q - 1, k * size + to], dst_ref=rx.at[whose, me],
                        send_sem=e_send, recv_sem=f_recv.at[q - 1, zone],
                        device_id={"expert": first + to}, device_id_type=MESH,
                    ).start()
                    return c2

                lax.fori_loop(1 if k == 0 else 0, size, one, 0)
            rx[whose, me] = out_ref[q - 1, lane]
            return c

        lax.fori_loop(1, dpn, one_peer, 0)

    def order_of(blocks):
        full = blocks * TILE
        at_row, at_col = iota((full, full), 0), iota((full, full), 1)
        per_cut = blocks * slot
        want = ((at_row % per_cut) // slot) * TILE + (at_row // per_cut) * slot + at_row % slot
        return (at_col == want).astype(F32).astype(BF16)

    def part_of(k, half):
        if half is None:
            return zone_of(k) * size, size, 0
        near = lane // (size // 2)
        side = near if half else (near + 1) % 2
        return zone_of(k) * size + side * (size // 2), size // 2, side

    count = size * TILE

    def natural(block):
        blocks = block.shape[0]
        count, per_cut, order = blocks * TILE, blocks * slot, order_of(blocks)
        pieces = [
            block[:, :, m * width : (m + 1) * width].reshape(count, width)
            for m in range(mains)
        ]
        if rest:
            sorted_rows = dot(order, block[:, :, base:].reshape(count, part)).astype(BF16)
            pieces.append(
                jnp.concatenate(
                    [sorted_rows[c * per_cut : (c + 1) * per_cut] for c in range(cuts)],
                    axis=1,
                )
            )
        return pieces

    def blocks_of(rows_out, blocks, store):
        count, order = blocks * TILE, order_of(blocks)
        for m in range(mains):
            store(
                m * width, width,
                rows_out[m * count : (m + 1) * count].reshape(blocks, TILE, width),
            )
        if rest:
            extra = rows_out[mains * count :]
            stacked = jnp.concatenate(
                [extra[:, c * part : (c + 1) * part] for c in range(cuts)], axis=0
            )
            mixed = dot(order, stacked, ((0,), (0,))).astype(BF16)
            store(base, part, mixed.reshape(blocks, TILE, part))

    def expert(block):
        x = jnp.concatenate(natural(block), axis=0)
        gate = dot(x, ffn_ref[0], ((1,), (1,)))
        up = dot(x, ffn_ref[1], ((1,), (1,)))
        hidden = (gate / (1.0 + jnp.exp(-gate)) * up).astype(BF16)
        return dot(hidden, ffn_ref[2])

    def partial_copy(j, t, half):
        first, blocks, _ = part_of(t, half)
        mine = pl.ds(first, blocks)
        return pltpu.make_async_remote_copy(
            src_ref=rx.at[peer_of(j), mine], dst_ref=px.at[dp, mine],
            send_sem=p_send, recv_sem=p_recv.at[dpn - 1 - j, zone_of(t), half or 0],
            device_id={"dp": peer_of(j)}, device_id_type=MESH,
        )

    def give_back(to, at):
        return pltpu.make_async_remote_copy(
            src_ref=fin.at[to], dst_ref=ret.at[at],
            send_sem=r_send, recv_sem=r_recv.at[at // size],
            device_id={"expert": to}, device_id_type=MESH,
        )

    def loss_copy(to, at):
        return pltpu.make_async_remote_copy(
            src_ref=zsnd, dst_ref=zrx.at[at],
            send_sem=z_send, recv_sem=z_recv,
            device_id={"expert": to}, device_id_type=MESH,
        )

    def loss_dp(j, whose):
        return pltpu.make_async_remote_copy(
            src_ref=zmid, dst_ref=zdp.at[whose],
            send_sem=y_send, recv_sem=y_recv,
            device_id={"dp": peer_of(j)}, device_id_type=MESH,
        )

    def route():
        inputs[2].wait()
        logits = dot(tok_ref[...], router_ref[...], ((1,), (1,)))
        top = jnp.max(logits, axis=1, keepdims=True)
        log_total = top + jnp.log(jnp.sum(jnp.exp(logits - top), axis=1, keepdims=True))
        local = jnp.sum(log_total * log_total, axis=0, keepdims=True)
        zsnd[...] = jnp.broadcast_to(local, zsnd.shape)
        zrx[me] = jnp.broadcast_to(local, zsnd.shape)

        def send_loss(j, c):
            loss_copy((me + j) % n, me).start()
            return c

        lax.fori_loop(1, n, send_loss, 0)

        same = (iota((n, n), 0) == iota((n, n), 1)).astype(F32).astype(BF16)
        hot = [dot(h.astype(F32).astype(BF16), same, ((0,), (0,))) > 0.5 for h in hot_t]
        ids = [
            jnp.sum(jnp.where(h, iota((rows, n), 1), 0), axis=1, keepdims=True) for h in hot
        ]
        chosen = [jnp.sum(jnp.where(h, logits, 0.0), axis=1, keepdims=True) for h in hot]
        high = functools.reduce(jnp.maximum, chosen)
        exps = [jnp.exp(c - high) for c in chosen]
        share = [e / sum(exps) for e in exps]
        all_hot = sum(h.astype(F32) for h in hot).astype(BF16)
        lower = (iota((rows, rows), 1) < iota((rows, rows), 0)).astype(F32).astype(BF16)
        before = dot(lower, all_hot)
        pos = [
            jnp.sum(jnp.where(h, before, 0.0), axis=1, keepdims=True).astype(jnp.int32)
            for h in hot
        ]
        goal = [targets(ids[k], pos[k]) for k in range(topk)]

        col_at = iota((rows, n * TILE), 1)
        for i in range(mains + (cuts if rest else 0)):
            w = sum(jnp.where(col_at == goal[k][i], share[k], 0.0) for k in range(topk))
            hi = w.astype(BF16)
            hi_ref[i] = hi
            lo_ref[i] = (w - hi.astype(F32)).astype(BF16)

    def arrive(k, part=None, onward=False):
        first = zone_of(k) * size

        def one(j, c):
            at = first + (lane + size - j) % size
            dispatch(at, at).wait_recv()
            for q in range(1, dpn if onward else 1):
                forward(q, at, dp).start()
            return c

        if part is None:
            lax.fori_loop(1 if home(k) else 0, size, one, 0)
        else:
            quarter = size // 4
            lax.fori_loop(part * quarter, (part + 1) * quarter, one, 0)

    def own_part(k):
        own[k] = expert(rx[dp, pl.ds(zone_of(k) * size, size)])

    def peer_part(k):
        first = zone_of(k) * size

        def one(q, c):
            whose = peer_of(q)

            come = pl.ds(first, size - 1 if home(k) else size)
            landed(rx.at[whose, come], f_recv.at[q - 1, zone_of(k)])
            out = expert(rx[whose, pl.ds(first, size)]).astype(BF16)

            def store(start, wide, value):
                rx[whose, pl.ds(first, size), :, start : start + wide] = value

            blocks_of(out, size, store)
            return c

        lax.fori_loop(1, dpn, one, 0)

    def send_part(k, half=None):
        for q in range(1, dpn):
            partial_copy(q, k, half).start()

    def finish(k, half=None):
        first, blocks, side = part_of(k, half)
        if half is None:
            total = own[k]
        else:
            total = []
            for at, tall in [(m * count, blocks * TILE) for m in range(mains)] + (
                [(mains * count, blocks * slot)] if rest else []
            ):
                total.append(own[k, pl.ds(pl.multiple_of(at + side * tall, 8), tall), :])
            total = jnp.concatenate(total, axis=0)
        for q in range(1, dpn):
            block = px.at[peer_of(q), pl.ds(first, blocks)]
            landed(block, p_recv.at[q - 1, zone_of(k), half or 0])
            total = total + jnp.concatenate(natural(block[...]), axis=0).astype(F32)

        def store(start, wide, value):
            fin[pl.ds(first, blocks), :, start : start + wide] = value

        blocks_of(total.astype(BF16), blocks, store)
        mixed = home(k) and half != 0

        def back(j, c):
            give_back(first + (lane % blocks + j) % blocks, me).start()
            return c

        lax.fori_loop(1 if mixed else 0, blocks, back, 0)
        if mixed:
            ret[me] = fin[me]

    def cut(i, k):
        start = zone_of(k) * size * TILE
        sub = (iota((n * TILE, size * TILE), 0) == iota((n * TILE, size * TILE), 1) + start)
        sub = sub.astype(F32).astype(BF16)
        hi = dot(hi_ref[i], sub).astype(BF16)
        lo = dot(lo_ref[i], sub).astype(BF16)
        return jnp.concatenate([hi, lo], axis=1)

    def weigh(k):
        for i in range(mains + (cuts if rest else 0)):
            for k in range(groups):
                w_ref[i, k] = cut(i, k)

    def take(k, place=""):
        here = pl.ds(zone_of(k) * size, size - 1 if home(k) else size)
        landed(ret.at[here], r_recv.at[zone_of(k)])

        def twice(x):
            return jnp.concatenate([x, x], axis=0)

        mine = pl.ds(zone_of(k) * size, size)
        for c in range(cuts):
            cols = slice(c * part, (c + 1) * part)
            acc = 0.0 if place in ("first", "only") else acc_ref[:, cols]
            for m in range(mains):
                seen = ret[mine, :, m * width + c * part : m * width + (c + 1) * part]
                acc = acc + dot(w_ref[m, k], twice(seen.reshape(count, part)))
            if rest:
                seen = ret[mine, :, base:].reshape(count, part)
                acc = acc + dot(w_ref[mains + c, k], twice(seen))
            if place in ("last", "only"):
                mix_ref[:, cols] = acc.astype(BF16)
            else:
                acc_ref[:, cols] = acc

    def loads_in(k):
        landed(ffn_ref, w_sem)

    def gather_loss():
        landed(zrx.at[pl.ds(0, n - 1)], z_recv)
        mid = zrx[0]
        for i in range(1, n):
            mid = mid + zrx[i]
        zmid[...] = mid
        zdp[dp] = mid

        for q in range(1, dpn):
            loss_dp(q, dp).start()

    def drain(k):
        landed(snd.at[pl.ds(0, n - 1)], d_send)
        landed(zrx.at[pl.ds(0, n - 1)], z_send)
        if groups > near:
            landed(rx.at[pl.ds(0, dpn - 1), pl.ds(0, (groups - near) * size)], f_send)
        landed(peer_tok, s_send)
        landed(peer_ids, t_send)
        landed(out_ref.at[pl.ds(0, dpn - 1), pl.ds(0, near * size - 1)], e_send)
        landed(px.at[pl.ds(0, dpn - 1)], p_send)
        landed(zdp.at[pl.ds(0, dpn - 1)], y_send)
        landed(zdp.at[pl.ds(0, dpn - 1)], y_recv)
        loss = zdp[dp]
        for q in range(1, dpn):
            loss = loss + zdp[peer_of(q)]
        zout[...] = loss[0:1, 0:1] / F32(rows * n * dpn)
        z_copy.start()

    steps = {
        "send": send_group, "got": arrive, "share": share, "relay": relay,
        "pass": functools.partial(arrive, onward=True),
        "own": own_part, "peer": peer_part,
        "part": send_part, "end": finish, "done": take, "load": loads_in,
        "route": lambda k: route(), "loss": lambda k: gather_loss(), "weigh": weigh, "drain": drain,
    }
    for op, at, *more in plan:
        with jax.named_scope(f"{op}_{at}_{more}"):
            split = any(isinstance(m, tuple) for m in more)
            if not (split or isinstance(at, tuple)):
                steps[op](at, *more)
            elif split or None in at or 0 in at:
                for kind in range(2):
                    first, *rest_of = [m[kind] if isinstance(m, tuple) else m for m in (at, *more)]
                    if first is not None:
                        pl.when(inner == kind)(functools.partial(steps[op], first, *rest_of))
            else:
                steps[op](at[0] + inner * (at[1] - at[0]), *more)

    z_copy.wait()

    landed(fin.at[pl.ds(0, n - 1)], r_send)


def on_device(n, dpn, tokens, router_weight, route_ids, gate_weight, up_weight, down_weight):
    rows, width = tokens.shape
    topk = route_ids.shape[1]
    experts = router_weight.shape[1]
    assert experts == n and gate_weight.shape[0] == 1
    cap = 5 * rows * topk // (4 * experts)
    groups = 4 if n % 4 == 0 else 1
    mains, rest = cap // TILE, cap % TILE
    slot = 1
    while slot < rest:
        slot *= 2
    block = mains * width + (width * slot // TILE if rest else 0)
    size = n // groups
    in_rows = size * TILE * mains + (size * slot if rest else 0)
    hidden = gate_weight.shape[1]
    vmem = pl.BlockSpec(memory_space=pltpu.VMEM)
    hbm = pl.BlockSpec(memory_space=pl.ANY)
    dma = pltpu.SemaphoreType.DMA
    mixture, loss = pl.pallas_call(
        functools.partial(kernel, n, dpn, cap, groups),
        out_shape=(
            pltpu.VMEM((rows, width), BF16),
            jax.ShapeDtypeStruct((1, 1), F32),
        ),
        in_specs=[hbm] * 6,
        out_specs=(vmem, hbm),
        scratch_shapes=[
            pltpu.VMEM((rows, width), BF16),
            pltpu.VMEM((experts, width), BF16),
            pltpu.VMEM((topk, rows), jnp.int32),
            pltpu.VMEM((n, TILE, block), BF16),
            pltpu.VMEM((dpn, n, TILE, block), BF16),
            pltpu.VMEM((dpn, n, TILE, block), BF16),
            pltpu.VMEM((n, TILE, block), BF16),
            pltpu.VMEM((n, TILE, block), BF16),
            pltpu.VMEM((groups, in_rows, width), F32),
            pltpu.VMEM((3, hidden, width), BF16),
            pltpu.VMEM((8, 128), F32),
            pltpu.VMEM((n, 8, 128), F32),
            pltpu.VMEM((8, 128), F32),
            pltpu.VMEM((dpn, 8, 128), F32),
            dma, dma((n,)), dma, dma((dpn - 1, groups)),
            dma, dma((dpn - 1, groups, 2)), dma, dma((groups,)),
            dma, dma, dma, dma, dma, dma((3,)),
            pltpu.VMEM((mains + (TILE // slot if rest else 0), rows, n * TILE), BF16),
            pltpu.VMEM((mains + (TILE // slot if rest else 0), rows, n * TILE), BF16),
            pltpu.VMEM((mains + (TILE // slot if rest else 0), groups, rows, 2 * size * TILE), BF16),
            pltpu.VMEM((rows, width), F32),
            pltpu.VMEM((1, 1), F32),
            dma,
            pltpu.VMEM((dpn - 1, rows, width), BF16),
            pltpu.VMEM((dpn - 1, topk, rows), jnp.int32),
            pltpu.VMEM((dpn - 1, (2 if groups == 4 else 1) * size, TILE, block), BF16),
            dma, dma((dpn - 1,)), dma, dma((dpn - 1,)), dma,
        ],
        compiler_params=pltpu.CompilerParams(
            collective_id=0, has_side_effects=True, vmem_limit_bytes=60 * 1024 * 1024
        ),
    )(tokens, router_weight.T, route_ids.T, gate_weight, up_weight, down_weight)
    return mixture, loss[0, 0]


def solution(mesh):
    in_specs = (
        P(("dp", "expert"), None),
        P(),
        P(("dp", "expert"), None),
        P("expert", "dp", None),
        P("expert", "dp", None),
        P("expert", "dp", None),
    )
    out_specs = (P(("dp", "expert"), None), P())
    return jax.shard_map(
        functools.partial(on_device, mesh.shape["expert"], mesh.shape["dp"]),
        mesh=mesh, in_specs=in_specs, out_specs=out_specs, check_vma=False,
    )
```

```python
import functools

import jax
import jax.numpy as jnp
from jax import lax
from jax.experimental import pallas as pl
from jax.experimental.pallas import tpu as pltpu
from jax.sharding import PartitionSpec as P

MESH = pl.DeviceIdType.MESH
F32 = jnp.float32
BF16 = jnp.bfloat16
TILE = 16
NO = None
PLAN = (
    ('share', 0, True),
    ('send', (2, 1)),
    ('share', 1),
    ('send', 0),
    ('send', (1, 2)),
    ('pass', (None, 2), 1),
    ('send', 3),
    ('load', (None, 0)),
    ('pass', (None, 2), 0),
    ('pass', (None, 2), 2),
    ('pass', (None, 2), 3),
    ('share', 2),
    ('share', 3),
    ('load', (0, None)),
    ('got', 0),
    ('own', 0),
    ('route', 0),
    ('got', (1, None)),
    ('pass', (2, None), 1),
    ('pass', (2, None), 0),
    ('own', (1, 2)),
    ('weigh', 0),
    ('pass', (2, None), 2),
    ('pass', (2, None), 3),
    ('peer', (None, 2)),
    ('part', (None, 2), 0),
    ('part', (None, 2), 1),
    ('relay', 0),
    ('got', (None, 1)),
    ('own', (2, 1)),
    ('pass', 3, 0),
    ('pass', 3, 1),
    ('end', (None, 2), 0),
    ('pass', 3, 2),
    ('end', (None, 2), 1),
    ('pass', 3, 3),
    ('peer', (2, None)),
    ('part', (2, None), 0),
    ('part', (2, None), 1),
    ('own', 3),
    ('peer', (3, 1)),
    ('part', (3, 1), 0),
    ('part', (3, 1), 1),
    ('end', (2, None), 0),
    ('peer', (1, 3)),
    ('part', (1, 3), 0),
    ('part', (None, 3), 1),
    ('peer', 0),
    ('part', 0, 0),
    ('part', (1, None), 1),
    ('part', 0, 1),
    ('end', (2, None), 1),
    ('end', (3, 1), 0),
    ('loss', (0, None)),
    ('end', (3, 1), 1),
    ('loss', (None, 0)),
    ('end', (1, 3), 0),
    ('end', (0, None), 0),
    ('end', (1, 3), 1),
    ('end', (None, 0), 0),
    ('done', 2, 'first'),
    ('end', 0, 1),
    ('drain', 0),
    ('done', (3, 1)),
    ('done', 0),
    ('done', (1, 3), 'last'),
)
ORDER_ONE = ("send", "load", "relay", "got", "route", "weigh", "own", "peer", "part", "end", "loss", "drain", "done")
PLAN_ONE = (("share", 0, True), ("share", 1), ("share", 2), ("share", 3)) + tuple(
    (op, 0, "only") if op == "done" else (op, 0) for op in ORDER_ONE
)


def dot(a, b, dims=((1,), (0,))):
    return lax.dot_general(a, b, (dims, ((), ())), preferred_element_type=F32)


def iota(shape, axis):
    return lax.broadcasted_iota(jnp.int32, shape, axis)


def kernel(
    n, dpn, cap, groups,
    tok_hbm, router_hbm, ids_hbm, gate_hbm, up_hbm, down_hbm,
    mix_ref, z_ref,
    tok_ref, router_ref, ids_ref, snd, rx, px, fin, ret, own, ffn_ref, zsnd, zrx, zmid, zdp,
    d_send, d_recv, f_send, f_recv, p_send, p_recv, r_send, r_recv,
    z_send, z_recv, y_send, y_recv, w_sem, i_sem,
    hi_ref, lo_ref, w_ref, acc_ref, zout, o_sem,
    peer_tok, peer_ids, out_ref, s_send, s_recv, t_send, t_recv, e_send,
):
    rows, width = tok_hbm.shape
    topk = ids_hbm.shape[0]
    size = n // groups
    mains = cap // TILE
    rest = cap - mains * TILE
    slot = 1
    while slot < rest:
        slot *= 2
    cuts = TILE // slot
    part = width // cuts
    base = mains * width
    me = lax.axis_index("expert")
    dp = lax.axis_index("dp")
    zone = me // size
    lane = me % size

    plan = PLAN if groups == 4 else PLAN_ONE
    inner = ((zone + 1) // 2) % 2 if groups == 4 else 0

    near = 2 if groups == 4 else 1

    def home(k):
        return isinstance(k, int) and k == 0

    def zone_of(k):
        if groups == 4:
            return ((zone // 2 + k // 2) % 2) * 2 + (zone % 2 + k % 2) % 2
        return (zone + k) % groups

    def peer_of(j):
        return (dp + j) % dpn

    def landed(ref, sem):
        pltpu.make_async_copy(ref, ref, sem).wait()

    inputs = [
        pltpu.make_async_copy(src, dst, i_sem.at[i])
        for i, (src, dst) in enumerate(
            ((ids_hbm, ids_ref), (tok_hbm, tok_ref), (router_hbm, router_ref))
        )
    ]
    for load in inputs:
        load.start()

    z_copy = pltpu.make_async_copy(zout, z_ref, o_sem)
    barrier = pltpu.get_barrier_semaphore()

    def greet(j, c):
        pl.semaphore_signal(
            barrier, inc=1, device_id={"expert": (me + j) % n}, device_id_type=MESH
        )
        return c

    lax.fori_loop(1, n, greet, 0)
    for j in range(1, dpn):
        pl.semaphore_signal(
            barrier, inc=1, device_id={"dp": peer_of(j)}, device_id_type=MESH
        )

    inputs[0].wait()
    upper = (iota((rows, rows), 0) < iota((rows, rows), 1)).astype(F32).astype(BF16)

    def hot_of(ids):
        return [(ids[k : k + 1, :] == iota((n, rows), 0)) for k in range(topk)]

    def goals(ids):
        hot = hot_of(ids)
        before = dot(sum(h.astype(F32) for h in hot).astype(BF16), upper)
        pos = [
            jnp.sum(jnp.where(h, before, 0.0), axis=0, keepdims=True).astype(jnp.int32)
            for h in hot
        ]
        return [targets(ids[k : k + 1, :], pos[k]) for k in range(topk)]

    def targets(ids, pos):
        out = []
        for m in range(mains):
            inside = (pos >= m * TILE) & (pos < (m + 1) * TILE)
            out.append(jnp.where(inside, ids * TILE + pos - m * TILE, -1))
        for c in range(cuts if rest else 0):
            inside = pos >= mains * TILE
            out.append(jnp.where(inside, ids * TILE + c * slot + pos - mains * TILE, -1))
        return out

    hot_t = hot_of(ids_ref[...])
    goal_t = goals(ids_ref[...])
    inputs[1].wait()
    for i, src in enumerate((gate_hbm, up_hbm, down_hbm)):
        pltpu.make_async_copy(src.at[0], ffn_ref.at[i], w_sem).start()
    row_at = iota((size * TILE, rows), 0)

    def dispatch(to, at):
        return pltpu.make_async_remote_copy(
            src_ref=snd.at[to], dst_ref=rx.at[dp, at],
            send_sem=d_send, recv_sem=d_recv.at[at],
            device_id={"expert": to}, device_id_type=MESH,
        )

    def forward(j, at, whose):
        return pltpu.make_async_remote_copy(
            src_ref=rx.at[dp, at], dst_ref=rx.at[whose, at],
            send_sem=f_send, recv_sem=f_recv.at[dpn - 1 - j, at // size],
            device_id={"dp": peer_of(j)}, device_id_type=MESH,
        )

    def gather(tokens, goal, first, store):
        def pick(i):
            at = row_at + first * TILE
            hit = at == goal[0][i]
            for c in range(1, topk):
                hit = hit | (at == goal[c][i])
            return hit.astype(F32).astype(BF16)

        for m in range(mains):
            chosen = dot(pick(m), tokens[...]).astype(BF16)
            store(m * width, width, chosen.reshape(size, TILE, width))
        if rest:
            extra = sum(
                dot(pick(mains + c), tokens[:, c * part : (c + 1) * part])
                for c in range(cuts)
            )
            store(base, part, extra.astype(BF16).reshape(size, TILE, part))

    def send_group(k):
        first = zone_of(k) * size

        def store(start, wide, value):
            snd[pl.ds(first, size), :, start : start + wide] = value

        gather(tok_ref, goal_t, first, store)

        def one(j, c):
            to = first + (lane + j) % size
            dispatch(to, me).start()
            return c

        lax.fori_loop(1 if home(k) else 0, size, one, 0)
        if home(k):
            rx[dp, me] = snd[me]

    def share(c, entry=False):
        if entry:
            pl.semaphore_wait(barrier, n - 1 + dpn - 1)
        mine = pl.ds(c * (rows // 4), rows // 4)
        for q in range(1, dpn):
            pltpu.make_async_remote_copy(
                src_ref=tok_ref.at[mine], dst_ref=peer_tok.at[dpn - 1 - q, mine],
                send_sem=s_send, recv_sem=s_recv.at[dpn - 1 - q],
                device_id={"dp": peer_of(q)}, device_id_type=MESH,
            ).start()
            if entry:
                pltpu.make_async_remote_copy(
                    src_ref=ids_ref, dst_ref=peer_ids.at[dpn - 1 - q],
                    send_sem=t_send, recv_sem=t_recv.at[dpn - 1 - q],
                    device_id={"dp": peer_of(q)}, device_id_type=MESH,
                ).start()

    def relay(unused):
        def one_peer(q, c):
            whose = peer_of(q)
            landed(peer_ids.at[q - 1], t_recv.at[q - 1])
            goal = goals(peer_ids[q - 1])
            landed(peer_tok.at[q - 1], s_recv.at[q - 1])
            for k in range(near):
                first = zone_of(k) * size

                def store(start, wide, value, k=k):
                    out_ref[q - 1, k * size : (k + 1) * size, :, start : start + wide] = value

                gather(peer_tok.at[q - 1], goal, first, store)

                def one(j, c2, k=k, first=first):
                    to = (lane + j) % size
                    pltpu.make_async_remote_copy(
                        src_ref=out_ref.at[q - 1, k * size + to], dst_ref=rx.at[whose, me],
                        send_sem=e_send, recv_sem=f_recv.at[q - 1, zone],
                        device_id={"expert": first + to}, device_id_type=MESH,
                    ).start()
                    return c2

                lax.fori_loop(1 if k == 0 else 0, size, one, 0)
            rx[whose, me] = out_ref[q - 1, lane]
            return c

        lax.fori_loop(1, dpn, one_peer, 0)

    def order_of(blocks):
        full = blocks * TILE
        at_row, at_col = iota((full, full), 0), iota((full, full), 1)
        per_cut = blocks * slot
        want = ((at_row % per_cut) // slot) * TILE + (at_row // per_cut) * slot + at_row % slot
        return (at_col == want).astype(F32).astype(BF16)

    def part_of(k, half):
        if half is None:
            return zone_of(k) * size, size, 0
        near = lane // (size // 2)
        side = near if half else (near + 1) % 2
        return zone_of(k) * size + side * (size // 2), size // 2, side

    count = size * TILE

    def natural(block):
        blocks = block.shape[0]
        count, per_cut, order = blocks * TILE, blocks * slot, order_of(blocks)
        pieces = [
            block[:, :, m * width : (m + 1) * width].reshape(count, width)
            for m in range(mains)
        ]
        if rest:
            sorted_rows = dot(order, block[:, :, base:].reshape(count, part)).astype(BF16)
            pieces.append(
                jnp.concatenate(
                    [sorted_rows[c * per_cut : (c + 1) * per_cut] for c in range(cuts)],
                    axis=1,
                )
            )
        return pieces

    def blocks_of(rows_out, blocks, store):
        count, order = blocks * TILE, order_of(blocks)
        for m in range(mains):
            store(
                m * width, width,
                rows_out[m * count : (m + 1) * count].reshape(blocks, TILE, width),
            )
        if rest:
            extra = rows_out[mains * count :]
            stacked = jnp.concatenate(
                [extra[:, c * part : (c + 1) * part] for c in range(cuts)], axis=0
            )
            mixed = dot(order, stacked, ((0,), (0,))).astype(BF16)
            store(base, part, mixed.reshape(blocks, TILE, part))

    def expert(block):
        x = jnp.concatenate(natural(block), axis=0)
        gate = dot(x, ffn_ref[0], ((1,), (1,)))
        up = dot(x, ffn_ref[1], ((1,), (1,)))
        hidden = (gate / (1.0 + jnp.exp(-gate)) * up).astype(BF16)
        return dot(hidden, ffn_ref[2])

    def partial_copy(j, t, half):
        first, blocks, _ = part_of(t, half)
        mine = pl.ds(first, blocks)
        return pltpu.make_async_remote_copy(
            src_ref=rx.at[peer_of(j), mine], dst_ref=px.at[dp, mine],
            send_sem=p_send, recv_sem=p_recv.at[dpn - 1 - j, zone_of(t), half or 0],
            device_id={"dp": peer_of(j)}, device_id_type=MESH,
        )

    def give_back(to, at):
        return pltpu.make_async_remote_copy(
            src_ref=fin.at[to], dst_ref=ret.at[at],
            send_sem=r_send, recv_sem=r_recv.at[at // size],
            device_id={"expert": to}, device_id_type=MESH,
        )

    def loss_copy(to, at):
        return pltpu.make_async_remote_copy(
            src_ref=zsnd, dst_ref=zrx.at[at],
            send_sem=z_send, recv_sem=z_recv,
            device_id={"expert": to}, device_id_type=MESH,
        )

    def loss_dp(j, whose):
        return pltpu.make_async_remote_copy(
            src_ref=zmid, dst_ref=zdp.at[whose],
            send_sem=y_send, recv_sem=y_recv,
            device_id={"dp": peer_of(j)}, device_id_type=MESH,
        )

    def route():
        inputs[2].wait()
        logits = dot(tok_ref[...], router_ref[...], ((1,), (1,)))
        top = jnp.max(logits, axis=1, keepdims=True)
        log_total = top + jnp.log(jnp.sum(jnp.exp(logits - top), axis=1, keepdims=True))
        local = jnp.sum(log_total * log_total, axis=0, keepdims=True)
        zsnd[...] = jnp.broadcast_to(local, zsnd.shape)
        zrx[me] = jnp.broadcast_to(local, zsnd.shape)

        def send_loss(j, c):
            loss_copy((me + j) % n, me).start()
            return c

        lax.fori_loop(1, n, send_loss, 0)

        same = (iota((n, n), 0) == iota((n, n), 1)).astype(F32).astype(BF16)
        hot = [dot(h.astype(F32).astype(BF16), same, ((0,), (0,))) > 0.5 for h in hot_t]
        ids = [
            jnp.sum(jnp.where(h, iota((rows, n), 1), 0), axis=1, keepdims=True) for h in hot
        ]
        chosen = [jnp.sum(jnp.where(h, logits, 0.0), axis=1, keepdims=True) for h in hot]
        high = functools.reduce(jnp.maximum, chosen)
        exps = [jnp.exp(c - high) for c in chosen]
        share = [e / sum(exps) for e in exps]
        all_hot = sum(h.astype(F32) for h in hot).astype(BF16)
        lower = (iota((rows, rows), 1) < iota((rows, rows), 0)).astype(F32).astype(BF16)
        before = dot(lower, all_hot)
        pos = [
            jnp.sum(jnp.where(h, before, 0.0), axis=1, keepdims=True).astype(jnp.int32)
            for h in hot
        ]
        goal = [targets(ids[k], pos[k]) for k in range(topk)]

        col_at = iota((rows, n * TILE), 1)
        for i in range(mains + (cuts if rest else 0)):
            w = sum(jnp.where(col_at == goal[k][i], share[k], 0.0) for k in range(topk))
            hi = w.astype(BF16)
            hi_ref[i] = hi
            lo_ref[i] = (w - hi.astype(F32)).astype(BF16)

    def arrive(k, part=None, onward=False):
        first = zone_of(k) * size

        def one(j, c):
            at = first + (lane + size - j) % size
            dispatch(at, at).wait_recv()
            for q in range(1, dpn if onward else 1):
                forward(q, at, dp).start()
            return c

        if part is None:
            lax.fori_loop(1 if home(k) else 0, size, one, 0)
        else:
            quarter = size // 4
            lax.fori_loop(part * quarter, (part + 1) * quarter, one, 0)

    def own_part(k):
        own[k] = expert(rx[dp, pl.ds(zone_of(k) * size, size)])

    def peer_part(k):
        first = zone_of(k) * size

        def one(q, c):
            whose = peer_of(q)

            come = pl.ds(first, size - 1 if home(k) else size)
            landed(rx.at[whose, come], f_recv.at[q - 1, zone_of(k)])
            out = expert(rx[whose, pl.ds(first, size)]).astype(BF16)

            def store(start, wide, value):
                rx[whose, pl.ds(first, size), :, start : start + wide] = value

            blocks_of(out, size, store)
            return c

        lax.fori_loop(1, dpn, one, 0)

    def send_part(k, half=None):
        for q in range(1, dpn):
            partial_copy(q, k, half).start()

    def finish(k, half=None):
        first, blocks, side = part_of(k, half)
        if half is None:
            total = own[k]
        else:
            total = []
            for at, tall in [(m * count, blocks * TILE) for m in range(mains)] + (
                [(mains * count, blocks * slot)] if rest else []
            ):
                total.append(own[k, pl.ds(pl.multiple_of(at + side * tall, 8), tall), :])
            total = jnp.concatenate(total, axis=0)
        for q in range(1, dpn):
            block = px.at[peer_of(q), pl.ds(first, blocks)]
            landed(block, p_recv.at[q - 1, zone_of(k), half or 0])
            total = total + jnp.concatenate(natural(block[...]), axis=0).astype(F32)

        def store(start, wide, value):
            fin[pl.ds(first, blocks), :, start : start + wide] = value

        blocks_of(total.astype(BF16), blocks, store)
        mixed = home(k) and half != 0

        def back(j, c):
            give_back(first + (lane % blocks + j) % blocks, me).start()
            return c

        lax.fori_loop(1 if mixed else 0, blocks, back, 0)
        if mixed:
            ret[me] = fin[me]

    def cut(i, k):
        start = zone_of(k) * size * TILE
        sub = (iota((n * TILE, size * TILE), 0) == iota((n * TILE, size * TILE), 1) + start)
        sub = sub.astype(F32).astype(BF16)
        hi = dot(hi_ref[i], sub).astype(BF16)
        lo = dot(lo_ref[i], sub).astype(BF16)
        return jnp.concatenate([hi, lo], axis=1)

    def weigh(k):
        for i in range(mains + (cuts if rest else 0)):
            for k in range(groups):
                w_ref[i, k] = cut(i, k)

    def take(k, place=""):
        here = pl.ds(zone_of(k) * size, size - 1 if home(k) else size)
        landed(ret.at[here], r_recv.at[zone_of(k)])

        def twice(x):
            return jnp.concatenate([x, x], axis=0)

        mine = pl.ds(zone_of(k) * size, size)
        for c in range(cuts):
            cols = slice(c * part, (c + 1) * part)
            acc = 0.0 if place in ("first", "only") else acc_ref[:, cols]
            for m in range(mains):
                seen = ret[mine, :, m * width + c * part : m * width + (c + 1) * part]
                acc = acc + dot(w_ref[m, k], twice(seen.reshape(count, part)))
            if rest:
                seen = ret[mine, :, base:].reshape(count, part)
                acc = acc + dot(w_ref[mains + c, k], twice(seen))
            if place in ("last", "only"):
                mix_ref[:, cols] = acc.astype(BF16)
            else:
                acc_ref[:, cols] = acc

    def loads_in(k):
        landed(ffn_ref, w_sem)

    def gather_loss():
        landed(zrx.at[pl.ds(0, n - 1)], z_recv)
        mid = zrx[0]
        for i in range(1, n):
            mid = mid + zrx[i]
        zmid[...] = mid
        zdp[dp] = mid

        for q in range(1, dpn):
            loss_dp(q, dp).start()

    def drain(k):
        landed(snd.at[pl.ds(0, n - 1)], d_send)
        landed(zrx.at[pl.ds(0, n - 1)], z_send)
        if groups > near:
            landed(rx.at[pl.ds(0, dpn - 1), pl.ds(0, (groups - near) * size)], f_send)
        landed(peer_tok, s_send)
        landed(peer_ids, t_send)
        landed(out_ref.at[pl.ds(0, dpn - 1), pl.ds(0, near * size - 1)], e_send)
        landed(px.at[pl.ds(0, dpn - 1)], p_send)
        landed(zdp.at[pl.ds(0, dpn - 1)], y_send)
        landed(zdp.at[pl.ds(0, dpn - 1)], y_recv)
        loss = zdp[dp]
        for q in range(1, dpn):
            loss = loss + zdp[peer_of(q)]
        zout[...] = loss[0:1, 0:1] / F32(rows * n * dpn)
        z_copy.start()

    steps = {
        "send": send_group, "got": arrive, "share": share, "relay": relay,
        "pass": functools.partial(arrive, onward=True),
        "own": own_part, "peer": peer_part,
        "part": send_part, "end": finish, "done": take, "load": loads_in,
        "route": lambda k: route(), "loss": lambda k: gather_loss(), "weigh": weigh, "drain": drain,
    }
    for op, at, *more in plan:
        with jax.named_scope(f"{op}_{at}_{more}"):
            split = any(isinstance(m, tuple) for m in more)
            if not (split or isinstance(at, tuple)):
                steps[op](at, *more)
            elif split or None in at or 0 in at:
                for kind in range(2):
                    first, *rest_of = [m[kind] if isinstance(m, tuple) else m for m in (at, *more)]
                    if first is not None:
                        pl.when(inner == kind)(functools.partial(steps[op], first, *rest_of))
            else:
                steps[op](at[0] + inner * (at[1] - at[0]), *more)

    z_copy.wait()

    landed(fin.at[pl.ds(0, n - 1)], r_send)


def on_device(n, dpn, tokens, router_weight, route_ids, gate_weight, up_weight, down_weight):
    rows, width = tokens.shape
    topk = route_ids.shape[1]
    experts = router_weight.shape[1]
    assert experts == n and gate_weight.shape[0] == 1
    cap = 5 * rows * topk // (4 * experts)
    groups = 4 if n % 4 == 0 else 1
    mains, rest = cap // TILE, cap % TILE
    slot = 1
    while slot < rest:
        slot *= 2
    block = mains * width + (width * slot // TILE if rest else 0)
    size = n // groups
    in_rows = size * TILE * mains + (size * slot if rest else 0)
    hidden = gate_weight.shape[1]
    vmem = pl.BlockSpec(memory_space=pltpu.VMEM)
    hbm = pl.BlockSpec(memory_space=pl.ANY)
    dma = pltpu.SemaphoreType.DMA
    mixture, loss = pl.pallas_call(
        functools.partial(kernel, n, dpn, cap, groups),
        out_shape=(
            pltpu.VMEM((rows, width), BF16),
            jax.ShapeDtypeStruct((1, 1), F32),
        ),
        in_specs=[hbm] * 6,
        out_specs=(vmem, hbm),
        scratch_shapes=[
            pltpu.VMEM((rows, width), BF16),
            pltpu.VMEM((experts, width), BF16),
            pltpu.VMEM((topk, rows), jnp.int32),
            pltpu.VMEM((n, TILE, block), BF16),
            pltpu.VMEM((dpn, n, TILE, block), BF16),
            pltpu.VMEM((dpn, n, TILE, block), BF16),
            pltpu.VMEM((n, TILE, block), BF16),
            pltpu.VMEM((n, TILE, block), BF16),
            pltpu.VMEM((groups, in_rows, width), F32),
            pltpu.VMEM((3, hidden, width), BF16),
            pltpu.VMEM((8, 128), F32),
            pltpu.VMEM((n, 8, 128), F32),
            pltpu.VMEM((8, 128), F32),
            pltpu.VMEM((dpn, 8, 128), F32),
            dma, dma((n,)), dma, dma((dpn - 1, groups)),
            dma, dma((dpn - 1, groups, 2)), dma, dma((groups,)),
            dma, dma, dma, dma, dma, dma((3,)),
            pltpu.VMEM((mains + (TILE // slot if rest else 0), rows, n * TILE), BF16),
            pltpu.VMEM((mains + (TILE // slot if rest else 0), rows, n * TILE), BF16),
            pltpu.VMEM((mains + (TILE // slot if rest else 0), groups, rows, 2 * size * TILE), BF16),
            pltpu.VMEM((rows, width), F32),
            pltpu.VMEM((1, 1), F32),
            dma,
            pltpu.VMEM((dpn - 1, rows, width), BF16),
            pltpu.VMEM((dpn - 1, topk, rows), jnp.int32),
            pltpu.VMEM((dpn - 1, (2 if groups == 4 else 1) * size, TILE, block), BF16),
            dma, dma((dpn - 1,)), dma, dma((dpn - 1,)), dma,
        ],
        compiler_params=pltpu.CompilerParams(
            collective_id=0, has_side_effects=True, vmem_limit_bytes=60 * 1024 * 1024
        ),
    )(tokens, router_weight.T, route_ids.T, gate_weight, up_weight, down_weight)
    return mixture, loss[0, 0]


def solution(mesh):
    in_specs = (
        P(("dp", "expert"), None),
        P(),
        P(("dp", "expert"), None),
        P("expert", "dp", None),
        P("expert", "dp", None),
        P("expert", "dp", None),
    )
    out_specs = (P(("dp", "expert"), None), P())
    return jax.shard_map(
        functools.partial(on_device, mesh.shape["expert"], mesh.shape["dp"]),
        mesh=mesh, in_specs=in_specs, out_specs=out_specs, check_vma=False,
    )
```

```python
import functools

import jax
import jax.numpy as jnp
from jax import lax
from jax.experimental import pallas as pl
from jax.experimental.pallas import tpu as pltpu
from jax.sharding import PartitionSpec as P

MESH = pl.DeviceIdType.MESH
F32 = jnp.float32
BF16 = jnp.bfloat16
TILE = 16
NO = None
PLAN = (
    ('share', 0, True),
    ('send', (2, 1)),
    ('share', 1),
    ('send', 0),
    ('send', (1, 2)),
    ('pass', (None, 2), 1),
    ('send', 3),
    ('load', (None, 0)),
    ('pass', (None, 2), 0),
    ('share', 2),
    ('pass', (None, 2), 2),
    ('pass', (None, 2), 3),
    ('share', 3),
    ('load', (0, None)),
    ('got', 0),
    ('own', 0),
    ('route', 0),
    ('got', (1, None)),
    ('pass', (2, None), 1),
    ('pass', (2, None), 0),
    ('own', (1, 2)),
    ('weigh', 0),
    ('pass', (2, None), 2),
    ('pass', (2, None), 3),
    ('peer', (None, 2)),
    ('part', (None, 2), 0),
    ('part', (None, 2), 1),
    ('relay', 0),
    ('got', (None, 1)),
    ('own', (2, 1)),
    ('pass', 3, 0),
    ('pass', 3, 1),
    ('end', (None, 2), 0),
    ('pass', 3, 2),
    ('end', (None, 2), 1),
    ('pass', 3, 3),
    ('peer', (2, None)),
    ('part', (2, None), 0),
    ('part', (2, None), 1),
    ('own', 3),
    ('peer', (3, 1)),
    ('part', (3, 1), 0),
    ('part', (3, 1), 1),
    ('end', (2, None), 0),
    ('peer', (1, 3)),
    ('part', (1, 3), 0),
    ('part', (None, 3), 1),
    ('peer', 0),
    ('part', 0, 0),
    ('part', (1, None), 1),
    ('part', 0, 1),
    ('end', (2, None), 1),
    ('end', (3, 1), 0),
    ('loss', (0, None)),
    ('end', (3, 1), 1),
    ('loss', (None, 0)),
    ('end', (1, 3), 0),
    ('end', (0, None), 0),
    ('end', (1, 3), 1),
    ('end', (None, 0), 0),
    ('done', 2, 'first'),
    ('end', 0, 1),
    ('drain', 0),
    ('done', (3, 1)),
    ('done', 0),
    ('done', (1, 3), 'last'),
)
ORDER_ONE = ("send", "load", "relay", "got", "route", "weigh", "own", "peer", "part", "end", "loss", "drain", "done")
PLAN_ONE = (("share", 0, True), ("share", 1), ("share", 2), ("share", 3)) + tuple(
    (op, 0, "only") if op == "done" else (op, 0) for op in ORDER_ONE
)


def dot(a, b, dims=((1,), (0,))):
    return lax.dot_general(a, b, (dims, ((), ())), preferred_element_type=F32)


def iota(shape, axis):
    return lax.broadcasted_iota(jnp.int32, shape, axis)


def kernel(
    n, dpn, cap, groups,
    tok_hbm, router_hbm, ids_hbm, gate_hbm, up_hbm, down_hbm,
    mix_ref, z_ref,
    tok_ref, router_ref, ids_ref, snd, rx, px, fin, ret, own, ffn_ref, zsnd, zrx, zmid, zdp,
    d_send, d_recv, f_send, f_recv, p_send, p_recv, r_send, r_recv,
    z_send, z_recv, y_send, y_recv, w_sem, i_sem,
    hi_ref, lo_ref, w_ref, acc_ref, zout, o_sem,
    peer_tok, peer_ids, out_ref, s_send, s_recv, t_send, t_recv, e_send,
):
    rows, width = tok_hbm.shape
    topk = ids_hbm.shape[0]
    size = n // groups
    mains = cap // TILE
    rest = cap - mains * TILE
    slot = 1
    while slot < rest:
        slot *= 2
    cuts = TILE // slot
    part = width // cuts
    base = mains * width
    me = lax.axis_index("expert")
    dp = lax.axis_index("dp")
    zone = me // size
    lane = me % size

    plan = PLAN if groups == 4 else PLAN_ONE
    inner = ((zone + 1) // 2) % 2 if groups == 4 else 0

    near = 2 if groups == 4 else 1

    def home(k):
        return isinstance(k, int) and k == 0

    def zone_of(k):
        if groups == 4:
            return ((zone // 2 + k // 2) % 2) * 2 + (zone % 2 + k % 2) % 2
        return (zone + k) % groups

    def peer_of(j):
        return (dp + j) % dpn

    def landed(ref, sem):
        pltpu.make_async_copy(ref, ref, sem).wait()

    inputs = [
        pltpu.make_async_copy(src, dst, i_sem.at[i])
        for i, (src, dst) in enumerate(
            ((ids_hbm, ids_ref), (tok_hbm, tok_ref), (router_hbm, router_ref))
        )
    ]
    for load in inputs:
        load.start()

    z_copy = pltpu.make_async_copy(zout, z_ref, o_sem)
    barrier = pltpu.get_barrier_semaphore()

    def greet(j, c):
        pl.semaphore_signal(
            barrier, inc=1, device_id={"expert": (me + j) % n}, device_id_type=MESH
        )
        return c

    lax.fori_loop(1, n, greet, 0)
    for j in range(1, dpn):
        pl.semaphore_signal(
            barrier, inc=1, device_id={"dp": peer_of(j)}, device_id_type=MESH
        )

    inputs[0].wait()
    upper = (iota((rows, rows), 0) < iota((rows, rows), 1)).astype(F32).astype(BF16)

    def hot_of(ids):
        return [(ids[k : k + 1, :] == iota((n, rows), 0)) for k in range(topk)]

    def goals(ids):
        hot = hot_of(ids)
        before = dot(sum(h.astype(F32) for h in hot).astype(BF16), upper)
        pos = [
            jnp.sum(jnp.where(h, before, 0.0), axis=0, keepdims=True).astype(jnp.int32)
            for h in hot
        ]
        return [targets(ids[k : k + 1, :], pos[k]) for k in range(topk)]

    def targets(ids, pos):
        out = []
        for m in range(mains):
            inside = (pos >= m * TILE) & (pos < (m + 1) * TILE)
            out.append(jnp.where(inside, ids * TILE + pos - m * TILE, -1))
        for c in range(cuts if rest else 0):
            inside = pos >= mains * TILE
            out.append(jnp.where(inside, ids * TILE + c * slot + pos - mains * TILE, -1))
        return out

    hot_t = hot_of(ids_ref[...])
    goal_t = goals(ids_ref[...])
    inputs[1].wait()
    for i, src in enumerate((gate_hbm, up_hbm, down_hbm)):
        pltpu.make_async_copy(src.at[0], ffn_ref.at[i], w_sem).start()
    row_at = iota((size * TILE, rows), 0)

    def dispatch(to, at):
        return pltpu.make_async_remote_copy(
            src_ref=snd.at[to], dst_ref=rx.at[dp, at],
            send_sem=d_send, recv_sem=d_recv.at[at],
            device_id={"expert": to}, device_id_type=MESH,
        )

    def forward(j, at, whose):
        return pltpu.make_async_remote_copy(
            src_ref=rx.at[dp, at], dst_ref=rx.at[whose, at],
            send_sem=f_send, recv_sem=f_recv.at[dpn - 1 - j, at // size],
            device_id={"dp": peer_of(j)}, device_id_type=MESH,
        )

    def gather(tokens, goal, first, store):
        def pick(i):
            at = row_at + first * TILE
            hit = at == goal[0][i]
            for c in range(1, topk):
                hit = hit | (at == goal[c][i])
            return hit.astype(F32).astype(BF16)

        for m in range(mains):
            chosen = dot(pick(m), tokens[...]).astype(BF16)
            store(m * width, width, chosen.reshape(size, TILE, width))
        if rest:
            extra = sum(
                dot(pick(mains + c), tokens[:, c * part : (c + 1) * part])
                for c in range(cuts)
            )
            store(base, part, extra.astype(BF16).reshape(size, TILE, part))

    def send_group(k):
        first = zone_of(k) * size

        def store(start, wide, value):
            snd[pl.ds(first, size), :, start : start + wide] = value

        gather(tok_ref, goal_t, first, store)

        def one(j, c):
            to = first + (lane + j) % size
            dispatch(to, me).start()
            return c

        lax.fori_loop(1 if home(k) else 0, size, one, 0)
        if home(k):
            rx[dp, me] = snd[me]

    def share(c, entry=False):
        if entry:
            pl.semaphore_wait(barrier, n - 1 + dpn - 1)
        mine = pl.ds(c * (rows // 4), rows // 4)
        for q in range(1, dpn):
            pltpu.make_async_remote_copy(
                src_ref=tok_ref.at[mine], dst_ref=peer_tok.at[dpn - 1 - q, mine],
                send_sem=s_send, recv_sem=s_recv.at[dpn - 1 - q],
                device_id={"dp": peer_of(q)}, device_id_type=MESH,
            ).start()
            if entry:
                pltpu.make_async_remote_copy(
                    src_ref=ids_ref, dst_ref=peer_ids.at[dpn - 1 - q],
                    send_sem=t_send, recv_sem=t_recv.at[dpn - 1 - q],
                    device_id={"dp": peer_of(q)}, device_id_type=MESH,
                ).start()

    def relay(unused):
        def one_peer(q, c):
            whose = peer_of(q)
            landed(peer_ids.at[q - 1], t_recv.at[q - 1])
            goal = goals(peer_ids[q - 1])
            landed(peer_tok.at[q - 1], s_recv.at[q - 1])
            for k in range(near):
                first = zone_of(k) * size

                def store(start, wide, value, k=k):
                    out_ref[q - 1, k * size : (k + 1) * size, :, start : start + wide] = value

                gather(peer_tok.at[q - 1], goal, first, store)

                def one(j, c2, k=k, first=first):
                    to = (lane + j) % size
                    pltpu.make_async_remote_copy(
                        src_ref=out_ref.at[q - 1, k * size + to], dst_ref=rx.at[whose, me],
                        send_sem=e_send, recv_sem=f_recv.at[q - 1, zone],
                        device_id={"expert": first + to}, device_id_type=MESH,
                    ).start()
                    return c2

                lax.fori_loop(1 if k == 0 else 0, size, one, 0)
            rx[whose, me] = out_ref[q - 1, lane]
            return c

        lax.fori_loop(1, dpn, one_peer, 0)

    def order_of(blocks):
        full = blocks * TILE
        at_row, at_col = iota((full, full), 0), iota((full, full), 1)
        per_cut = blocks * slot
        want = ((at_row % per_cut) // slot) * TILE + (at_row // per_cut) * slot + at_row % slot
        return (at_col == want).astype(F32).astype(BF16)

    def part_of(k, half):
        if half is None:
            return zone_of(k) * size, size, 0
        near = lane // (size // 2)
        side = near if half else (near + 1) % 2
        return zone_of(k) * size + side * (size // 2), size // 2, side

    count = size * TILE

    def natural(block):
        blocks = block.shape[0]
        count, per_cut, order = blocks * TILE, blocks * slot, order_of(blocks)
        pieces = [
            block[:, :, m * width : (m + 1) * width].reshape(count, width)
            for m in range(mains)
        ]
        if rest:
            sorted_rows = dot(order, block[:, :, base:].reshape(count, part)).astype(BF16)
            pieces.append(
                jnp.concatenate(
                    [sorted_rows[c * per_cut : (c + 1) * per_cut] for c in range(cuts)],
                    axis=1,
                )
            )
        return pieces

    def blocks_of(rows_out, blocks, store):
        count, order = blocks * TILE, order_of(blocks)
        for m in range(mains):
            store(
                m * width, width,
                rows_out[m * count : (m + 1) * count].reshape(blocks, TILE, width),
            )
        if rest:
            extra = rows_out[mains * count :]
            stacked = jnp.concatenate(
                [extra[:, c * part : (c + 1) * part] for c in range(cuts)], axis=0
            )
            mixed = dot(order, stacked, ((0,), (0,))).astype(BF16)
            store(base, part, mixed.reshape(blocks, TILE, part))

    def expert(block):
        x = jnp.concatenate(natural(block), axis=0)
        gate = dot(x, ffn_ref[0], ((1,), (1,)))
        up = dot(x, ffn_ref[1], ((1,), (1,)))
        hidden = (gate / (1.0 + jnp.exp(-gate)) * up).astype(BF16)
        return dot(hidden, ffn_ref[2])

    def partial_copy(j, t, half):
        first, blocks, _ = part_of(t, half)
        mine = pl.ds(first, blocks)
        return pltpu.make_async_remote_copy(
            src_ref=rx.at[peer_of(j), mine], dst_ref=px.at[dp, mine],
            send_sem=p_send, recv_sem=p_recv.at[dpn - 1 - j, zone_of(t), half or 0],
            device_id={"dp": peer_of(j)}, device_id_type=MESH,
        )

    def give_back(to, at):
        return pltpu.make_async_remote_copy(
            src_ref=fin.at[to], dst_ref=ret.at[at],
            send_sem=r_send, recv_sem=r_recv.at[at // size],
            device_id={"expert": to}, device_id_type=MESH,
        )

    def loss_copy(to, at):
        return pltpu.make_async_remote_copy(
            src_ref=zsnd, dst_ref=zrx.at[at],
            send_sem=z_send, recv_sem=z_recv,
            device_id={"expert": to}, device_id_type=MESH,
        )

    def loss_dp(j, whose):
        return pltpu.make_async_remote_copy(
            src_ref=zmid, dst_ref=zdp.at[whose],
            send_sem=y_send, recv_sem=y_recv,
            device_id={"dp": peer_of(j)}, device_id_type=MESH,
        )

    def route():
        inputs[2].wait()
        logits = dot(tok_ref[...], router_ref[...], ((1,), (1,)))
        top = jnp.max(logits, axis=1, keepdims=True)
        log_total = top + jnp.log(jnp.sum(jnp.exp(logits - top), axis=1, keepdims=True))
        local = jnp.sum(log_total * log_total, axis=0, keepdims=True)
        zsnd[...] = jnp.broadcast_to(local, zsnd.shape)
        zrx[me] = jnp.broadcast_to(local, zsnd.shape)

        def send_loss(j, c):
            loss_copy((me + j) % n, me).start()
            return c

        lax.fori_loop(1, n, send_loss, 0)

        same = (iota((n, n), 0) == iota((n, n), 1)).astype(F32).astype(BF16)
        hot = [dot(h.astype(F32).astype(BF16), same, ((0,), (0,))) > 0.5 for h in hot_t]
        ids = [
            jnp.sum(jnp.where(h, iota((rows, n), 1), 0), axis=1, keepdims=True) for h in hot
        ]
        chosen = [jnp.sum(jnp.where(h, logits, 0.0), axis=1, keepdims=True) for h in hot]
        high = functools.reduce(jnp.maximum, chosen)
        exps = [jnp.exp(c - high) for c in chosen]
        share = [e / sum(exps) for e in exps]
        all_hot = sum(h.astype(F32) for h in hot).astype(BF16)
        lower = (iota((rows, rows), 1) < iota((rows, rows), 0)).astype(F32).astype(BF16)
        before = dot(lower, all_hot)
        pos = [
            jnp.sum(jnp.where(h, before, 0.0), axis=1, keepdims=True).astype(jnp.int32)
            for h in hot
        ]
        goal = [targets(ids[k], pos[k]) for k in range(topk)]

        col_at = iota((rows, n * TILE), 1)
        for i in range(mains + (cuts if rest else 0)):
            w = sum(jnp.where(col_at == goal[k][i], share[k], 0.0) for k in range(topk))
            hi = w.astype(BF16)
            hi_ref[i] = hi
            lo_ref[i] = (w - hi.astype(F32)).astype(BF16)

    def arrive(k, part=None, onward=False):
        first = zone_of(k) * size

        def one(j, c):
            at = first + (lane + size - j) % size
            dispatch(at, at).wait_recv()
            for q in range(1, dpn if onward else 1):
                forward(q, at, dp).start()
            return c

        if part is None:
            lax.fori_loop(1 if home(k) else 0, size, one, 0)
        else:
            quarter = size // 4
            lax.fori_loop(part * quarter, (part + 1) * quarter, one, 0)

    def own_part(k):
        own[k] = expert(rx[dp, pl.ds(zone_of(k) * size, size)])

    def peer_part(k):
        first = zone_of(k) * size

        def one(q, c):
            whose = peer_of(q)

            come = pl.ds(first, size - 1 if home(k) else size)
            landed(rx.at[whose, come], f_recv.at[q - 1, zone_of(k)])
            out = expert(rx[whose, pl.ds(first, size)]).astype(BF16)

            def store(start, wide, value):
                rx[whose, pl.ds(first, size), :, start : start + wide] = value

            blocks_of(out, size, store)
            return c

        lax.fori_loop(1, dpn, one, 0)

    def send_part(k, half=None):
        for q in range(1, dpn):
            partial_copy(q, k, half).start()

    def finish(k, half=None):
        first, blocks, side = part_of(k, half)
        if half is None:
            total = own[k]
        else:
            total = []
            for at, tall in [(m * count, blocks * TILE) for m in range(mains)] + (
                [(mains * count, blocks * slot)] if rest else []
            ):
                total.append(own[k, pl.ds(pl.multiple_of(at + side * tall, 8), tall), :])
            total = jnp.concatenate(total, axis=0)
        for q in range(1, dpn):
            block = px.at[peer_of(q), pl.ds(first, blocks)]
            landed(block, p_recv.at[q - 1, zone_of(k), half or 0])
            total = total + jnp.concatenate(natural(block[...]), axis=0).astype(F32)

        def store(start, wide, value):
            fin[pl.ds(first, blocks), :, start : start + wide] = value

        blocks_of(total.astype(BF16), blocks, store)
        mixed = home(k) and half != 0

        def back(j, c):
            give_back(first + (lane % blocks + j) % blocks, me).start()
            return c

        lax.fori_loop(1 if mixed else 0, blocks, back, 0)
        if mixed:
            ret[me] = fin[me]

    def cut(i, k):
        start = zone_of(k) * size * TILE
        sub = (iota((n * TILE, size * TILE), 0) == iota((n * TILE, size * TILE), 1) + start)
        sub = sub.astype(F32).astype(BF16)
        hi = dot(hi_ref[i], sub).astype(BF16)
        lo = dot(lo_ref[i], sub).astype(BF16)
        return jnp.concatenate([hi, lo], axis=1)

    def weigh(k):
        for i in range(mains + (cuts if rest else 0)):
            for k in range(groups):
                w_ref[i, k] = cut(i, k)

    def take(k, place=""):
        here = pl.ds(zone_of(k) * size, size - 1 if home(k) else size)
        landed(ret.at[here], r_recv.at[zone_of(k)])

        def twice(x):
            return jnp.concatenate([x, x], axis=0)

        mine = pl.ds(zone_of(k) * size, size)
        for c in range(cuts):
            cols = slice(c * part, (c + 1) * part)
            acc = 0.0 if place in ("first", "only") else acc_ref[:, cols]
            for m in range(mains):
                seen = ret[mine, :, m * width + c * part : m * width + (c + 1) * part]
                acc = acc + dot(w_ref[m, k], twice(seen.reshape(count, part)))
            if rest:
                seen = ret[mine, :, base:].reshape(count, part)
                acc = acc + dot(w_ref[mains + c, k], twice(seen))
            if place in ("last", "only"):
                mix_ref[:, cols] = acc.astype(BF16)
            else:
                acc_ref[:, cols] = acc

    def loads_in(k):
        landed(ffn_ref, w_sem)

    def gather_loss():
        landed(zrx.at[pl.ds(0, n - 1)], z_recv)
        mid = zrx[0]
        for i in range(1, n):
            mid = mid + zrx[i]
        zmid[...] = mid
        zdp[dp] = mid

        for q in range(1, dpn):
            loss_dp(q, dp).start()

    def drain(k):
        landed(snd.at[pl.ds(0, n - 1)], d_send)
        landed(zrx.at[pl.ds(0, n - 1)], z_send)
        if groups > near:
            landed(rx.at[pl.ds(0, dpn - 1), pl.ds(0, (groups - near) * size)], f_send)
        landed(peer_tok, s_send)
        landed(peer_ids, t_send)
        landed(out_ref.at[pl.ds(0, dpn - 1), pl.ds(0, near * size - 1)], e_send)
        landed(px.at[pl.ds(0, dpn - 1)], p_send)
        landed(zdp.at[pl.ds(0, dpn - 1)], y_send)
        landed(zdp.at[pl.ds(0, dpn - 1)], y_recv)
        loss = zdp[dp]
        for q in range(1, dpn):
            loss = loss + zdp[peer_of(q)]
        zout[...] = loss[0:1, 0:1] / F32(rows * n * dpn)
        z_copy.start()

    steps = {
        "send": send_group, "got": arrive, "share": share, "relay": relay,
        "pass": functools.partial(arrive, onward=True),
        "own": own_part, "peer": peer_part,
        "part": send_part, "end": finish, "done": take, "load": loads_in,
        "route": lambda k: route(), "loss": lambda k: gather_loss(), "weigh": weigh, "drain": drain,
    }
    for op, at, *more in plan:
        with jax.named_scope(f"{op}_{at}_{more}"):
            split = any(isinstance(m, tuple) for m in more)
            if not (split or isinstance(at, tuple)):
                steps[op](at, *more)
            elif split or None in at or 0 in at:
                for kind in range(2):
                    first, *rest_of = [m[kind] if isinstance(m, tuple) else m for m in (at, *more)]
                    if first is not None:
                        pl.when(inner == kind)(functools.partial(steps[op], first, *rest_of))
            else:
                steps[op](at[0] + inner * (at[1] - at[0]), *more)

    z_copy.wait()

    landed(fin.at[pl.ds(0, n - 1)], r_send)


def on_device(n, dpn, tokens, router_weight, route_ids, gate_weight, up_weight, down_weight):
    rows, width = tokens.shape
    topk = route_ids.shape[1]
    experts = router_weight.shape[1]
    assert experts == n and gate_weight.shape[0] == 1
    cap = 5 * rows * topk // (4 * experts)
    groups = 4 if n % 4 == 0 else 1
    mains, rest = cap // TILE, cap % TILE
    slot = 1
    while slot < rest:
        slot *= 2
    block = mains * width + (width * slot // TILE if rest else 0)
    size = n // groups
    in_rows = size * TILE * mains + (size * slot if rest else 0)
    hidden = gate_weight.shape[1]
    vmem = pl.BlockSpec(memory_space=pltpu.VMEM)
    hbm = pl.BlockSpec(memory_space=pl.ANY)
    dma = pltpu.SemaphoreType.DMA
    mixture, loss = pl.pallas_call(
        functools.partial(kernel, n, dpn, cap, groups),
        out_shape=(
            pltpu.VMEM((rows, width), BF16),
            jax.ShapeDtypeStruct((1, 1), F32),
        ),
        in_specs=[hbm] * 6,
        out_specs=(vmem, hbm),
        scratch_shapes=[
            pltpu.VMEM((rows, width), BF16),
            pltpu.VMEM((experts, width), BF16),
            pltpu.VMEM((topk, rows), jnp.int32),
            pltpu.VMEM((n, TILE, block), BF16),
            pltpu.VMEM((dpn, n, TILE, block), BF16),
            pltpu.VMEM((dpn, n, TILE, block), BF16),
            pltpu.VMEM((n, TILE, block), BF16),
            pltpu.VMEM((n, TILE, block), BF16),
            pltpu.VMEM((groups, in_rows, width), F32),
            pltpu.VMEM((3, hidden, width), BF16),
            pltpu.VMEM((8, 128), F32),
            pltpu.VMEM((n, 8, 128), F32),
            pltpu.VMEM((8, 128), F32),
            pltpu.VMEM((dpn, 8, 128), F32),
            dma, dma((n,)), dma, dma((dpn - 1, groups)),
            dma, dma((dpn - 1, groups, 2)), dma, dma((groups,)),
            dma, dma, dma, dma, dma, dma((3,)),
            pltpu.VMEM((mains + (TILE // slot if rest else 0), rows, n * TILE), BF16),
            pltpu.VMEM((mains + (TILE // slot if rest else 0), rows, n * TILE), BF16),
            pltpu.VMEM((mains + (TILE // slot if rest else 0), groups, rows, 2 * size * TILE), BF16),
            pltpu.VMEM((rows, width), F32),
            pltpu.VMEM((1, 1), F32),
            dma,
            pltpu.VMEM((dpn - 1, rows, width), BF16),
            pltpu.VMEM((dpn - 1, topk, rows), jnp.int32),
            pltpu.VMEM((dpn - 1, (2 if groups == 4 else 1) * size, TILE, block), BF16),
            dma, dma((dpn - 1,)), dma, dma((dpn - 1,)), dma,
        ],
        compiler_params=pltpu.CompilerParams(
            collective_id=0, has_side_effects=True, vmem_limit_bytes=60 * 1024 * 1024
        ),
    )(tokens, router_weight.T, route_ids.T, gate_weight, up_weight, down_weight)
    return mixture, loss[0, 0]


def solution(mesh):
    in_specs = (
        P(("dp", "expert"), None),
        P(),
        P(("dp", "expert"), None),
        P("expert", "dp", None),
        P("expert", "dp", None),
        P("expert", "dp", None),
    )
    out_specs = (P(("dp", "expert"), None), P())
    return jax.shard_map(
        functools.partial(on_device, mesh.shape["expert"], mesh.shape["dp"]),
        mesh=mesh, in_specs=in_specs, out_specs=out_specs, check_vma=False,
    )
```
